16 devices in a mesh: data: 2 (over y, z), tp: 8 (over x, core).
Axes of the slice: x: 4, y: 2, z: 1, core: 2. Of those that a mesh axis runs over, the one named last changes fastest.
The devices are a block of a 4x4x8 slice.
Arguments:
- x_tokens: bfloat16 [8192, 4096], P(('data', 'tp')), parts along dimension 0
- ln_gamma: float32 [4096], replicated
- w_qkv: bfloat16 [4096, 32, 384], P(None, 'tp')
- w_out: bfloat16 [32, 128, 4096], P('tp')
- w_up: bfloat16 [4096, 11008], P(None, 'tp')
- w_down: bfloat16 [11008, 4096], P('tp')
Outputs:
- output: bfloat16 [8192, 4096], P(('data', 'tp')), parts along dimension 0
There are 2 independent parts. The reference program is written for one: setup_inputs(seed, part) draws one part's arguments, and reference() takes and returns one part's arrays. A program takes and returns all parts, laid end to end along the dimension named above; an argument that names none is the same for every part.
All inputs are finite; a program needn't handle non-finite values.
Results may differ from the reference program's by a relative error of at most 0.00288605.
Values are sent between devices in bfloat16 or wider.
A program may use at most 768 MiB of HBM per device.

```python
import math
import jax
import jax.numpy as jnp
from jax import lax

SEQ_LEN = 4096
MODEL_DIM = 4096
FF_DIM = 11008
NUM_HEADS = 32
HEAD_DIM = MODEL_DIM // NUM_HEADS
BLOCK_ROWS = min(SEQ_LEN, 256)
N_BLOCKS = SEQ_LEN // BLOCK_ROWS
ATTN_SCALE = HEAD_DIM ** -0.5
LN_EPS = 1e-6
QK_GAIN = max(math.log(SEQ_LEN) - 2.0, 1.0) ** 0.25


def setup_inputs(seed: int = 0, part: int = 0) -> dict:
    rand_keys = jax.random.split(jax.random.key(seed), 6)
    tokens = jax.random.normal(jax.random.fold_in(rand_keys[0], part), (SEQ_LEN, MODEL_DIM), jnp.float32)
    ln_gain = 1.0 + 0.5 * jax.random.normal(rand_keys[1], (MODEL_DIM,), jnp.float32)
    qkv_gain = jnp.array([QK_GAIN, QK_GAIN, 1.0], jnp.float32).reshape(1, 1, 3, 1)
    w_qkv = jax.random.normal(rand_keys[2], (MODEL_DIM, NUM_HEADS, 3, HEAD_DIM), jnp.float32) * qkv_gain * MODEL_DIM ** -0.5
    w_out = jax.random.normal(rand_keys[3], (NUM_HEADS, HEAD_DIM, MODEL_DIM), jnp.float32) * (2.0 * MODEL_DIM ** -0.5)
    w_up = jax.random.normal(rand_keys[4], (MODEL_DIM, FF_DIM), jnp.float32) * MODEL_DIM ** -0.5
    w_down = jax.random.normal(rand_keys[5], (FF_DIM, MODEL_DIM), jnp.float32) * (1.5 * FF_DIM ** -0.5)
    return {
        "x_tokens": tokens.astype(jnp.bfloat16),
        "ln_gamma": ln_gain,
        "w_qkv": w_qkv.reshape(MODEL_DIM, NUM_HEADS, 3 * HEAD_DIM).astype(jnp.bfloat16),
        "w_out": w_out.astype(jnp.bfloat16),
        "w_up": w_up.astype(jnp.bfloat16),
        "w_down": w_down.astype(jnp.bfloat16),
    }


def layer_norm(row_vals, ln_gain):
    row_mean = jnp.mean(row_vals, axis=-1, keepdims=True)
    centered = row_vals - row_mean
    row_var = jnp.mean(centered * centered, axis=-1, keepdims=True)
    return centered * lax.rsqrt(row_var + LN_EPS) * ln_gain


def reference(x_tokens, ln_gamma, w_qkv, w_out, w_up, w_down):
    residual = x_tokens.astype(jnp.float32)
    normed = layer_norm(residual, ln_gamma).astype(jnp.bfloat16)

    def head_step(attn_acc, head_weights):
        wqkv_head, wout_head = head_weights
        qkv_rows = jnp.dot(normed, wqkv_head, preferred_element_type=jnp.float32).astype(jnp.bfloat16)
        query_rows = qkv_rows[:, :HEAD_DIM]
        key_trans = qkv_rows[:, HEAD_DIM:2 * HEAD_DIM].T
        value_rows = qkv_rows[:, 2 * HEAD_DIM:]

        def query_block(query_blk):
            scores = jnp.dot(query_blk, key_trans, preferred_element_type=jnp.float32) * ATTN_SCALE
            row_max = jnp.max(scores, axis=-1, keepdims=True)
            exp_scores = jnp.exp(scores - row_max)
            exp_sum = jnp.sum(exp_scores, axis=-1, keepdims=True)
            block_out = jnp.dot(exp_scores.astype(jnp.bfloat16), value_rows, preferred_element_type=jnp.float32)
            return (block_out / exp_sum).astype(jnp.bfloat16)

        head_out = lax.map(query_block, query_rows.reshape(N_BLOCKS, BLOCK_ROWS, HEAD_DIM)).reshape(SEQ_LEN, HEAD_DIM)
        return attn_acc + jnp.dot(head_out, wout_head, preferred_element_type=jnp.float32), None

    attn_init = jnp.zeros((SEQ_LEN, MODEL_DIM), jnp.float32)
    attn_sum = lax.scan(head_step, attn_init, (jnp.moveaxis(w_qkv, 1, 0), w_out))[0]

    def mlp_block(row_blk):
        pre_act = jnp.dot(row_blk, w_up, preferred_element_type=jnp.float32)
        hidden = jax.nn.gelu(pre_act, approximate=True).astype(jnp.bfloat16)
        return jnp.dot(hidden, w_down, preferred_element_type=jnp.float32)

    mlp_sum = lax.map(mlp_block, normed.reshape(N_BLOCKS, BLOCK_ROWS, MODEL_DIM)).reshape(SEQ_LEN, MODEL_DIM)
    return (residual + attn_sum + mlp_sum).astype(jnp.bfloat16)
```

```python
import functools
import math

import jax
import jax.numpy as jnp
from jax import lax
from jax.experimental import pallas as pl
from jax.experimental.pallas import tpu as pltpu
from jax.sharding import PartitionSpec as P

LN_EPS = 1e-6
MESH = pl.DeviceIdType.MESH
CORES = 2
PIECE = 64
BLOCK = 256
COLS = 512
VMEM_LIMIT = 67_000_000
ANY = pl.BlockSpec(memory_space=pl.ANY)


def norm_kernel(x_ref, g_ref, o_ref):
    vals = x_ref[...].astype(jnp.float32)
    centered = vals - jnp.mean(vals, axis=-1, keepdims=True)
    var = jnp.mean(centered * centered, axis=-1, keepdims=True)
    o_ref[...] = (centered * lax.rsqrt(var + LN_EPS) * g_ref[...]).astype(o_ref.dtype)


def layer_norm(x_loc, ln_gamma):
    rows, width = x_loc.shape
    tile = min(rows, 128)
    return pl.pallas_call(
        norm_kernel,
        grid=(rows // tile,),
        in_specs=[pl.BlockSpec((tile, width), lambda i: (i, 0)), pl.BlockSpec((1, width), lambda i: (0, 0))],
        out_specs=pl.BlockSpec((tile, width), lambda i: (i, 0)),
        out_shape=jax.ShapeDtypeStruct(x_loc.shape, jnp.bfloat16),
        name="norm",
    )(x_loc, ln_gamma.reshape(1, width))


def neighbours(chips):
    me = lax.axis_index("tp")
    chip, core = me // CORES, me % CORES
    right = (chip + 1) % chips * CORES + core
    left = (chip + chips - 1) % chips * CORES + core
    partner = chip * CORES + (1 - core)
    return me, chip, core, right, left, partner


def greet(devices):
    barrier = pltpu.get_barrier_semaphore()
    for device in devices:
        pl.semaphore_signal(barrier, inc=1, device_id={"tp": device}, device_id_type=MESH)
    pl.semaphore_wait(barrier, len(devices))


def remote(src, dst, send_sem, recv_sem, device):
    return pltpu.make_async_remote_copy(
        src_ref=src, dst_ref=dst, send_sem=send_sem, recv_sem=recv_sem, device_id={"tp": device}, device_id_type=MESH
    )


def each(count, body):
    def step(i, carry):
        body(i)
        return carry

    lax.fori_loop(0, count, step, 0)


def gather_kernel(
    chips, x_ref, wq_ref, w1_ref, xg_ref, qkv_ref, h_ref, wq_v, w1_v, lhs, qo, ho,
    w_sem, lhs_sem, qo_sem, ho_sem, send_r, recv_l, send_l, recv_r, send_p, recv_p,
):
    me, chip, core, right, left, partner = neighbours(chips)
    chunk = x_ref.shape[0]
    own_pieces = chunk // PIECE
    half = own_pieces // 2
    arrivals = own_pieces + half
    per_group = BLOCK // PIECE
    own_groups = chunk // BLOCK
    first = own_groups * CORES
    groups = first + arrivals

    greet((right, left, partner))

    load_q = pltpu.make_async_copy(wq_ref, wq_v, w_sem.at[0])
    load_1 = pltpu.make_async_copy(w1_ref, w1_v, w_sem.at[1])

    def own_piece(piece):
        return x_ref.at[pl.ds(pl.multiple_of(piece * PIECE, PIECE), PIECE)]

    def rows_at(device, piece):
        return pl.ds(pl.multiple_of(device * chunk + piece * PIECE, PIECE), PIECE)

    def to_right(j):
        return remote(own_piece(j), xg_ref.at[rows_at(me, j)], send_r.at[j], recv_l.at[j], right)

    def to_left(j):
        piece = (j + half) % own_pieces
        return remote(own_piece(piece), xg_ref.at[rows_at(me, piece)], send_l.at[j], recv_r.at[j], left)

    own_to_partner = remote(
        x_ref, xg_ref.at[pl.ds(pl.multiple_of(me * chunk, chunk), chunk)],
        send_p.at[2 * arrivals], recv_p.at[2 * arrivals], partner,
    )

    def start_own(j):
        to_right(j).start()
        to_left(j).start()

    own_to_partner.start()
    each(own_pieces, start_own)

    def from_left(j, c):
        return rows_at((chip + chips - 1 - j // own_pieces) % chips * CORES + c, j % own_pieces)

    def from_right(j, c):
        return rows_at((chip + 1 + j // own_pieces) % chips * CORES + c, (j + half) % own_pieces)

    def group_rows(g, i):
        j = g - first
        in_chunk = (g % own_groups) * per_group + i
        dev = jnp.where(g < own_groups, me, partner)
        early = dev * chunk + in_chunk * PIECE
        c = core if i < 2 else 1 - core
        if i % 2 == 0:
            late = ((chip + chips - 1 - j // own_pieces) % chips * CORES + c) * chunk + j % own_pieces * PIECE
        else:
            late = ((chip + 1 + j // own_pieces) % chips * CORES + c) * chunk + (j + half) % own_pieces * PIECE
        return early, late

    def lhs_copy(src, slot, i):
        return pltpu.make_async_copy(src, lhs.at[slot, pl.ds(i * PIECE, PIECE)], lhs_sem.at[slot, i])

    def relay_left(j):
        return remote(
            xg_ref.at[from_left(j, core)], xg_ref.at[from_left(j, core)],
            send_r.at[own_pieces + j], recv_l.at[own_pieces + j], right,
        )

    def relay_right(j):
        return remote(
            xg_ref.at[from_right(j, core)], xg_ref.at[from_right(j, core)],
            send_l.at[own_pieces + j], recv_r.at[own_pieces + j], left,
        )

    def share(j, side):
        rows = from_left(j, core) if side == 0 else from_right(j, core)
        return remote(xg_ref.at[rows], xg_ref.at[rows], send_p.at[2 * j + side], recv_p.at[2 * j + side], partner)

    def shared(j, side):
        rows = from_left(j, 1 - core) if side == 0 else from_right(j, 1 - core)
        return remote(xg_ref.at[rows], xg_ref.at[rows], send_p.at[2 * j + side], recv_p.at[2 * j + side], partner)

    def landed(rows, sem):
        return remote(xg_ref.at[rows], xg_ref.at[rows], sem, sem, partner)

    def fetch_links(g):
        slot = g % 2

        @pl.when(g < own_groups)
        def _():
            for i in range(per_group):
                lhs_copy(own_piece(g * per_group + i), slot, i).start()

        @pl.when((g >= own_groups) & (g < first))
        def _():
            @pl.when(g == own_groups)
            def _():
                own_to_partner.wait_recv()

            for i in range(per_group):
                lhs_copy(xg_ref.at[rows_at(partner, (g - own_groups) * per_group + i)], slot, i).start()

        @pl.when(g >= first)
        def _():
            j = g - first
            landed(from_left(j, core), recv_l.at[j]).wait_recv()
            landed(from_right(j, core), recv_r.at[j]).wait_recv()

            @pl.when(j < half)
            def _():
                relay_left(j).start()
                relay_right(j).start()

            share(j, 0).start()
            share(j, 1).start()
            lhs_copy(xg_ref.at[from_left(j, core)], slot, 0).start()
            lhs_copy(xg_ref.at[from_right(j, core)], slot, 1).start()

    def fetch_partner(g):
        @pl.when(g >= first)
        def _():
            j = g - first
            slot = g % 2
            shared(j, 0).wait_recv()
            shared(j, 1).wait_recv()
            lhs_copy(xg_ref.at[from_left(j, 1 - core)], slot, 2).start()
            lhs_copy(xg_ref.at[from_right(j, 1 - core)], slot, 3).start()

    def out_copies(g, i):
        slot = g % 2
        early, late = group_rows(g, i)
        rows = pl.ds(pl.multiple_of(jnp.where(g < first, early, late), PIECE), PIECE)
        part = pl.ds(i * PIECE, PIECE)
        return (
            pltpu.make_async_copy(qo.at[slot, part], qkv_ref.at[rows], qo_sem.at[slot, i]),
            pltpu.make_async_copy(ho.at[slot, part], h_ref.at[rows], ho_sem.at[slot, i]),
        )

    def wait_out(g):
        for i in range(per_group):
            for copy in out_copies(g, i):
                copy.wait()

    qkv_width = wq_v.shape[1]
    ff_width = w1_v.shape[0]

    def compute(g):
        slot = g % 2
        for i in range(per_group):
            lhs_copy(own_piece(i), slot, i).wait()

        @pl.when(g >= 2)
        def _():
            wait_out(g - 2)

        @pl.when(g == 0)
        def _():
            load_q.wait()

        def qkv_tile(n):
            cols = pl.ds(pl.multiple_of(n * COLS, COLS), COLS)
            qo[slot, :, cols] = jnp.dot(lhs[slot], wq_v[:, cols], preferred_element_type=jnp.float32).astype(qo.dtype)

        each(qkv_width // COLS, qkv_tile)

        @pl.when(g == 0)
        def _():
            load_1.wait()

        def up(rows):
            pre = lax.dot_general(lhs[slot], w1_v[rows, :], (((1,), (1,)), ((), ())), preferred_element_type=jnp.float32)
            return jax.nn.gelu(pre, approximate=True).astype(ho.dtype)

        def up_tile(n):
            cols = pl.ds(pl.multiple_of(n * COLS, COLS), COLS)
            ho[slot, :, cols] = up(cols)

        each(ff_width // COLS, up_tile)
        done = ff_width // COLS * COLS
        if done < ff_width:
            ho[slot, :, done:] = up(pl.ds(done, ff_width - done))
        for i in range(per_group):
            for copy in out_copies(g, i):
                copy.start()

    load_q.start()
    load_1.start()
    fetch_links(jnp.int32(0))

    def step(g):
        @pl.when(g < groups - 3)
        def _():
            fetch_links(g + 1)

        compute(g)

        @pl.when((g >= groups - 3) & (g < groups - 1))
        def _():
            fetch_links(g + 1)

        @pl.when(g < groups - 1)
        def _():
            fetch_partner(g + 1)

    each(groups, step)

    wait_out(jnp.int32(groups - 2))
    wait_out(jnp.int32(groups - 1))
    own_to_partner.wait_send()

    def finish_own(j):
        to_right(j).wait_send()
        to_left(j).wait_send()

    def finish_relay(j):
        relay_left(j).wait_send()
        relay_right(j).wait_send()

    def finish_share(j):
        share(j, 0).wait_send()
        share(j, 1).wait_send()

    each(own_pieces, finish_own)
    each(half, finish_relay)
    each(arrivals, finish_share)


def gather_project(chips, normed, w_qkv, w_up_t):
    chunk, width = normed.shape
    tokens = chunk * chips * CORES
    qkv_width, ff_width = w_qkv.shape[1], w_up_t.shape[0]
    arrivals = chunk // PIECE + chunk // PIECE // 2
    dma = pltpu.SemaphoreType.DMA
    out = pl.pallas_call(
        functools.partial(gather_kernel, chips),
        in_specs=[ANY] * 3,
        out_specs=[ANY] * 3,
        out_shape=[
            jax.ShapeDtypeStruct((tokens, width), jnp.bfloat16),
            jax.ShapeDtypeStruct((tokens, qkv_width), jnp.bfloat16),
            jax.ShapeDtypeStruct((tokens, ff_width), jnp.bfloat16),
        ],
        scratch_shapes=[
            pltpu.VMEM(w_qkv.shape, jnp.bfloat16),
            pltpu.VMEM(w_up_t.shape, jnp.bfloat16),
            pltpu.VMEM((2, BLOCK, width), jnp.bfloat16),
            pltpu.VMEM((2, BLOCK, qkv_width), jnp.bfloat16),
            pltpu.VMEM((2, BLOCK, ff_width), jnp.bfloat16),
            dma((2,)), dma((2, BLOCK // PIECE)), dma((2, BLOCK // PIECE)), dma((2, BLOCK // PIECE)),
            dma((arrivals,)), dma((arrivals,)), dma((arrivals,)), dma((arrivals,)),
            dma((2 * arrivals + 1,)), dma((2 * arrivals + 1,)),
        ],
        compiler_params=pltpu.CompilerParams(collective_id=0, has_side_effects=True, vmem_limit_bytes=VMEM_LIMIT),
        name="gather_project",
    )(normed, w_qkv, w_up_t)
    return out[1], out[2]


def attend_kernel(
    chips, heads, head_dim, qkv_ref, h_ref, x_ref, wo_ref, w2_ref,
    y_ref, rp_ref, ro_ref, rn_ref, ps_ref,
    qkv_v, wo_v, w2_v, s_v, o_v, h_v, acc, stage, x_v, y_v,
    w_sem, h_sem, st_sem, x_sem, y_sem, ps_sem, send_p, recv_p, send_o, recv_o, send_n, recv_n,
):
    me, chip, core, right, left, partner = neighbours(chips)
    chunk, width = x_ref.shape
    tokens = qkv_v.shape[0]
    blocks = chunk // BLOCK
    pairs = chips * blocks
    half = width // 2
    slices = BLOCK // PIECE
    key_tile = min(tokens, 1024)
    factor = head_dim ** -0.5 * math.log2(math.e)

    greet((right, left, partner))

    load_qkv = pltpu.make_async_copy(qkv_ref, qkv_v, w_sem.at[0])
    load_wo = pltpu.make_async_copy(wo_ref, wo_v, w_sem.at[1])
    load_w2 = pltpu.make_async_copy(w2_ref, w2_v, w_sem.at[2])
    load_qkv.start()
    load_wo.start()
    load_w2.start()

    def place(p):
        quarter = p // blocks
        mid = (quarter + 1) // 2 % 2
        offset = mid * (1 + 2 * (p % 2)) + (1 - mid) * (2 - 2 * (quarter // 3))
        block = mid * (quarter - 1) + (1 - mid) * (p % 2)
        return offset, block

    def block_rows(i, size=BLOCK):
        return pl.ds(pl.multiple_of(i * size, size), size)

    def token_block(s):
        p = s // 2
        offset, block = place(p)
        device = (chip + offset) % chips * CORES + (core + 1 - s % 2) % 2
        return device * blocks + block

    def to_partner(p):
        return remote(acc.at[0], rp_ref.at[block_rows(p)], send_p.at[p], recv_p.at[p], partner)

    def to_side(p, side):
        src = ps_ref.at[block_rows(p), pl.ds(side * half, half)]
        dst = ro_ref.at[block_rows(side * blocks + p)]
        return remote(src, dst, send_o.at[side, p], recv_o.at[side, p], left if side else right)

    def to_owner(p, k):
        side = p % 2
        offset, block = place(p)
        src = ps_ref.at[block_rows(p * slices + k, PIECE)]
        dst = rn_ref.at[block_rows((side * blocks + block) * slices + k, PIECE)]
        device = (chip + offset) % chips * CORES + core
        return remote(src, dst, send_n.at[side, block * slices + k], recv_n.at[side, block * slices + k], device)

    def owner_part(side, block, k):
        rows = block_rows((side * blocks + block) * slices + k, PIECE)
        return rn_ref.at[rows], recv_n.at[side, block * slices + k]

    def attend_head(row, head):
        base = pl.multiple_of(head * 3 * head_dim, head_dim)
        q = qkv_v[row, pl.ds(base, head_dim)]
        k_cols = pl.ds(pl.multiple_of(base + head_dim, head_dim), head_dim)
        v_cols = pl.ds(pl.multiple_of(base + 2 * head_dim, head_dim), head_dim)
        top = None
        for t in range(tokens // key_tile):
            keys = pl.ds(t * key_tile, key_tile)
            s = lax.dot_general(q, qkv_v[keys, k_cols], (((1,), (1,)), ((), ())), preferred_element_type=jnp.float32)
            s_v[:, keys] = s
            tile_top = jnp.max(s, axis=-1, keepdims=True)
            top = tile_top if top is None else jnp.maximum(top, tile_top)
        total, out = None, None
        for t in range(tokens // key_tile):
            keys = pl.ds(t * key_tile, key_tile)
            e = jnp.exp2((s_v[:, keys] - top) * factor)
            tile_sum = jnp.sum(e, axis=-1, keepdims=True)
            tile_out = jnp.dot(e.astype(jnp.bfloat16), qkv_v[keys, v_cols], preferred_element_type=jnp.float32)
            total = tile_sum if total is None else total + tile_sum
            out = tile_out if out is None else out + tile_out
        o_v[:, pl.ds(pl.multiple_of(head * head_dim, head_dim), head_dim)] = (out / total).astype(o_v.dtype)

    def load_h(s):
        return pltpu.make_async_copy(h_ref.at[block_rows(token_block(s))], h_v, h_sem)

    def stage_partner(p):
        return pltpu.make_async_copy(rp_ref.at[block_rows(p)], stage.at[0], st_sem.at[0])

    def stage_side(side, block):
        return pltpu.make_async_copy(
            ro_ref.at[block_rows(side * blocks + block)], stage.at[1, :, pl.ds(0, half)], st_sem.at[1]
        )

    def spill(p):
        return pltpu.make_async_copy(acc.at[1], ps_ref.at[block_rows(p)], ps_sem)

    def step(s):
        p = s // 2
        mine = s % 2
        offset, block = place(p)
        is_mid = (offset % 2) == 1
        load_h(s).start()

        @pl.when(s == 0)
        def _():
            load_qkv.wait()

        row = block_rows(token_block(s))
        each(heads, lambda head: attend_head(row, head))
        load_h(s).wait()

        @pl.when(s == 0)
        def _():
            load_wo.wait()
            load_w2.wait()

        @pl.when((mine == 0) & (p > 0))
        def _():
            to_partner(p - 1).wait_send()

        @pl.when(mine == 1)
        def _():
            to_partner(p).wait_recv()
            stage_partner(p).start()

            @pl.when(is_mid)
            def _():
                side = p % 2
                pltpu.make_async_remote_copy(
                    src_ref=ro_ref.at[block_rows(side * blocks + block)], dst_ref=ro_ref.at[block_rows(side * blocks + block)],
                    send_sem=send_o.at[side, block], recv_sem=recv_o.at[side, block],
                    device_id={"tp": partner}, device_id_type=MESH,
                ).wait_recv()
                stage_side(side, block).start()

        def project(n):
            cols = pl.ds(pl.multiple_of(n * COLS, COLS), COLS)
            acc[mine, :, cols] = jnp.dot(
                o_v[...], wo_v[:, cols], preferred_element_type=jnp.float32
            ) + jnp.dot(h_v[...], w2_v[:, cols], preferred_element_type=jnp.float32)

        each(width // COLS, project)

        @pl.when(mine == 0)
        def _():
            to_partner(p).start()

        @pl.when(mine == 1)
        def _():
            stage_partner(p).wait()

            def add(n):
                cols = pl.ds(pl.multiple_of(n * COLS, COLS), COLS)
                acc[1, :, cols] += stage[0, :, cols]

            each(width // COLS, add)

            @pl.when(is_mid)
            def _():
                side = p % 2
                stage_side(side, block).wait()

                def add_side(n):
                    dst = pl.ds(pl.multiple_of(side * half + n * COLS, COLS), COLS)
                    src = pl.ds(pl.multiple_of(n * COLS, COLS), COLS)
                    acc[1, :, dst] += stage[1, :, src]

                each(half // COLS, add_side)

            @pl.when(offset != 0)
            def _():
                spill(p).start()
                spill(p).wait()

                @pl.when(is_mid)
                def _():
                    each(slices, lambda k: to_owner(p, k).start())

                @pl.when(offset == 2)
                def _():
                    to_side(p, 0).start()
                    to_side(p, 1).start()

            @pl.when(offset == 0)
            def _():
                def final(k):
                    rows = block_rows(block * slices + k, PIECE)
                    load_x = pltpu.make_async_copy(x_ref.at[rows], x_v, x_sem)
                    load_x.start()
                    copies = []
                    for side in range(2):
                        src, sem = owner_part(side, block, k)
                        remote(src, src, sem, sem, partner).wait_recv()
                        copy = pltpu.make_async_copy(src, stage.at[side, pl.ds(0, PIECE)], st_sem.at[side])
                        copy.start()
                        copies.append(copy)
                    load_x.wait()
                    for copy in copies:
                        copy.wait()

                    def finish(n):
                        cols = pl.ds(pl.multiple_of(n * COLS, COLS), COLS)
                        summed = acc[1, block_rows(k, PIECE), cols] + stage[0, pl.ds(0, PIECE), cols] + stage[1, pl.ds(0, PIECE), cols]
                        y_v[:, cols] = (x_v[:, cols].astype(jnp.float32) + summed).astype(y_v.dtype)

                    each(width // COLS, finish)
                    store = pltpu.make_async_copy(y_v, y_ref.at[rows], y_sem)
                    store.start()
                    store.wait()

                each(slices, final)

    each(2 * pairs, step)
    to_partner(pairs - 1).wait_send()
    for p in range(blocks):
        to_side(p, 0).wait_send()
        to_side(p, 1).wait_send()
    for p in range(blocks, 3 * blocks):
        each(slices, lambda k, p=p: to_owner(p, k).wait_send())


def attend_reduce(chips, heads, head_dim, qkv, hidden, x_loc, w_out, w_down):
    chunk, width = x_loc.shape
    tokens, qkv_width = qkv.shape
    ff_width = hidden.shape[1]
    blocks = chunk // BLOCK
    slices = BLOCK // PIECE
    pairs = chips * blocks
    f32 = jnp.float32
    dma = pltpu.SemaphoreType.DMA
    out = pl.pallas_call(
        functools.partial(attend_kernel, chips, heads, head_dim),
        in_specs=[ANY] * 5,
        out_specs=[ANY] * 5,
        out_shape=[
            jax.ShapeDtypeStruct((chunk, width), jnp.bfloat16),
            jax.ShapeDtypeStruct((pairs * BLOCK, width), f32),
            jax.ShapeDtypeStruct((2 * chunk, width // 2), f32),
            jax.ShapeDtypeStruct((2 * chunk, width), f32),
            jax.ShapeDtypeStruct((3 * chunk, width), f32),
        ],
        scratch_shapes=[
            pltpu.VMEM((tokens, qkv_width), jnp.bfloat16),
            pltpu.VMEM(w_out.shape, jnp.bfloat16),
            pltpu.VMEM(w_down.shape, jnp.bfloat16),
            pltpu.VMEM((BLOCK, tokens), f32),
            pltpu.VMEM((BLOCK, w_out.shape[0]), jnp.bfloat16),
            pltpu.VMEM((BLOCK, ff_width), jnp.bfloat16),
            pltpu.VMEM((2, BLOCK, width), f32),
            pltpu.VMEM((2, BLOCK, width), f32),
            pltpu.VMEM((PIECE, width), jnp.bfloat16),
            pltpu.VMEM((PIECE, width), jnp.bfloat16),
            dma((3,)), dma, dma((2,)), dma, dma, dma,
            dma((pairs,)), dma((pairs,)),
            dma((2, blocks)), dma((2, blocks)),
            dma((2, blocks * slices)), dma((2, blocks * slices)),
        ],
        compiler_params=pltpu.CompilerParams(collective_id=1, has_side_effects=True, vmem_limit_bytes=VMEM_LIMIT),
        name="attend_reduce",
    )(qkv, hidden, x_loc, w_out, w_down)
    return out[0]


def solution(mesh):
    chips = mesh.shape["tp"] // CORES

    def local_block(x_loc, ln_gamma, w_qkv, w_out, w_up, w_down):
        model_dim = x_loc.shape[1]
        heads, head_dim = w_out.shape[0], w_out.shape[1]
        normed = layer_norm(x_loc, ln_gamma)
        qkv, hidden = gather_project(chips, normed, w_qkv.reshape(model_dim, heads * 3 * head_dim), w_up.T)
        return attend_reduce(chips, heads, head_dim, qkv, hidden, x_loc, w_out.reshape(heads * head_dim, model_dim), w_down)

    row_spec = P(("data", "tp"), None)
    return jax.shard_map(local_block, mesh=mesh, in_specs=(row_spec, P(None), P(None, "tp", None), P("tp", None, None), P(None, "tp"), P("tp", None)), out_specs=row_spec, check_vma=False)
```

```python
import functools
import math

import jax
import jax.numpy as jnp
from jax import lax
from jax.experimental import pallas as pl
from jax.experimental.pallas import tpu as pltpu
from jax.sharding import PartitionSpec as P

LN_EPS = 1e-6
MESH = pl.DeviceIdType.MESH
CORES = 2
PIECE = 64
GROUP = 256
BLOCK = 256
FIRST = 128
REPACK = 256
LATE = 3
COLS = 2048
LANES = 512
VMEM_LIMIT = 67_000_000
ANY = pl.BlockSpec(memory_space=pl.ANY)


def neighbours(chips):
    me = lax.axis_index("tp")
    chip, core = me // CORES, me % CORES
    right = (chip + 1) % chips * CORES + core
    left = (chip + chips - 1) % chips * CORES + core
    partner = chip * CORES + (1 - core)
    return me, chip, core, right, left, partner


def greet(devices):
    barrier = pltpu.get_barrier_semaphore()
    for device in devices:
        pl.semaphore_signal(barrier, inc=1, device_id={"tp": device}, device_id_type=MESH)
    pl.semaphore_wait(barrier, len(devices))


def remote(src, dst, send_sem, recv_sem, device):
    return pltpu.make_async_remote_copy(
        src_ref=src, dst_ref=dst, send_sem=send_sem, recv_sem=recv_sem, device_id={"tp": device}, device_id_type=MESH
    )


def each(count, body):
    def step(i, carry):
        body(i)
        return carry

    lax.fori_loop(0, count, step, 0)


def block_kernel(
    chips, x_ref, gamma_ref, wq_ref, wo_ref, w1_ref, w2_ref,
    y_ref, xg_ref, h_ref, rp_ref, ro_ref, rn_ref, ps_ref,
    qkv_v, wo_v, w2_v, gamma_v,
    w_sem, x_sem, wq_sem, lhs_sem, ho_sem, send_r, recv_l, send_l, recv_r, send_g, recv_g,
    h_sem, st_sem, xr_sem, y_sem, ps_sem, send_p, recv_p, send_o, recv_o, send_n, recv_n,
):
    me, chip, core, right, left, partner = neighbours(chips)
    chunk, width = x_ref.shape
    heads, qkv_head = wq_ref.shape[1], wq_ref.shape[2]
    load_wo = pltpu.make_async_copy(wo_ref, wo_v, w_sem.at[1])
    load_w2 = pltpu.make_async_copy(w2_ref, w2_v, w_sem.at[2])
    bf16, f32 = jnp.bfloat16, jnp.float32

    def project_phase(wq_v, w1_v, w4_v, lhs, ho):
        own_pieces = chunk // PIECE
        half = own_pieces // 2
        arrivals = own_pieces + half
        per_group = GROUP // PIECE
        own_groups = chunk // GROUP
        first = own_groups * CORES
        groups = first + arrivals

        load_x = [pltpu.make_async_copy(x_ref.at[pl.ds(i * GROUP, GROUP)], lhs.at[i], x_sem.at[i]) for i in range(own_groups)]
        for copy in load_x:
            copy.start()
        load_gamma = pltpu.make_async_copy(gamma_ref, gamma_v, w_sem.at[3])
        load_gamma.start()

        def load_wq(i):
            rows = pl.ds(pl.multiple_of(i * REPACK, REPACK), REPACK)
            return pltpu.make_async_copy(wq_ref.at[rows], w4_v.at[i % 2], wq_sem.at[i % 2])

        load_w1 = pltpu.make_async_copy(w1_ref, w1_v, w_sem.at[0])
        load_wq(0).start()
        load_w1.start()
        greet((right, left, partner))

        def rows_at(device, piece):
            return pl.ds(pl.multiple_of(device * chunk + piece * PIECE, PIECE), PIECE)

        def own_send(piece, sends, recvs, j, device):
            rows = xg_ref.at[rows_at(me, piece)]
            return remote(rows, rows, sends.at[j], recvs.at[j], device)

        def to_right(j):
            return own_send(j, send_r, recv_l, j, right)

        def to_left(j):
            return own_send((j + half) % own_pieces, send_l, recv_r, j, left)

        def own_to_partner():
            rows = xg_ref.at[pl.ds(pl.multiple_of(me * chunk, chunk), chunk)]
            return remote(rows, rows, send_g.at[2 * arrivals], recv_g.at[2 * arrivals], partner)

        def normalise(j):
            out = []
            for side in range(2):
                rows = pl.ds(pl.multiple_of(j * PIECE, PIECE), PIECE)
                vals = lhs[side, rows, :].astype(f32)
                centered = vals - jnp.mean(vals, axis=-1, keepdims=True)
                var = jnp.mean(centered * centered, axis=-1, keepdims=True)
                lhs[side, rows, :] = (centered * lax.rsqrt(var + LN_EPS) * gamma_v[...]).astype(bf16)
                piece = j + side * half
                copy = pltpu.make_async_copy(lhs.at[side, rows], xg_ref.at[rows_at(me, piece)], lhs_sem.at[side, 0])
                copy.start()
                out.append(copy)
            for copy in out:
                copy.wait()

        for copy in load_x:
            copy.wait()
        load_gamma.wait()

        def open_links(j):
            normalise(j)
            to_right(j).start()
            to_left(j).start()

        each(half, open_links)
        own_to_partner().start()

        def open_rest(j):
            to_right(half + j).start()
            to_left(half + j).start()

        each(half, open_rest)
        load_wo.start()
        load_w2.start()

        def repack(i):
            @pl.when(i < width // REPACK - 1)
            def _():
                load_wq(i + 1).start()

            load_wq(i).wait()
            rows = pl.ds(pl.multiple_of(i * REPACK, REPACK), REPACK)
            wq_v[rows, :] = w4_v[i % 2].reshape(REPACK, heads * qkv_head)

        each(width // REPACK, repack)
        load_w1.wait()

        def left_row(j, c):
            return ((chip + chips - 1 - j // own_pieces) % chips * CORES + c) * chunk + j % own_pieces * PIECE

        def right_row(j, c):
            return ((chip + 1 + j // own_pieces) % chips * CORES + c) * chunk + (j + half) % own_pieces * PIECE

        def side_rows(j, side, c):
            row = right_row(j, c) if side else left_row(j, c)
            return pl.ds(pl.multiple_of(row, PIECE), PIECE)

        def lhs_copy(src, slot, i):
            return pltpu.make_async_copy(src, lhs.at[slot, pl.ds(i * PIECE, PIECE)], lhs_sem.at[slot, i])

        def relay(j, side):
            rows = xg_ref.at[side_rows(j, side, core)]
            sends, recvs, device = (send_l, recv_r, left) if side else (send_r, recv_l, right)
            return remote(rows, rows, sends.at[own_pieces + j], recvs.at[own_pieces + j], device)

        def share(j, side, c):
            rows = xg_ref.at[side_rows(j, side, c)]
            return remote(rows, rows, send_g.at[2 * j + side], recv_g.at[2 * j + side], partner)

        def fetch_links(g):
            slot = g % 2

            @pl.when((g >= own_groups) & (g < first))
            def _():
                @pl.when(g == own_groups)
                def _():
                    own_to_partner().wait_recv()

                for i in range(per_group):
                    lhs_copy(xg_ref.at[rows_at(partner, (g - own_groups) * per_group + i)], slot, i).start()

            @pl.when(g >= first)
            def _():
                j = g - first
                for side in range(2):
                    rows = xg_ref.at[side_rows(j, side, core)]
                    sem = (recv_r if side else recv_l).at[j]
                    remote(rows, rows, sem, sem, partner).wait_recv()

                @pl.when(j < half)
                def _():
                    relay(j, 0).start()
                    relay(j, 1).start()

                for side in range(2):
                    share(j, side, core).start()
                    lhs_copy(xg_ref.at[side_rows(j, side, core)], slot, side).start()

        def fetch_partner(g):
            @pl.when(g >= first)
            def _():
                j = g - first
                for side in range(2):
                    share(j, side, 1 - core).wait_recv()
                for side in range(2):
                    lhs_copy(xg_ref.at[side_rows(j, side, 1 - core)], g % 2, 2 + side).start()

        def group_row(g, i):
            j = g - first
            early = jnp.where(g < own_groups, me, partner) * chunk + ((g % own_groups) * per_group + i) * PIECE
            c = core if i < 2 else 1 - core
            late = right_row(j, c) if i % 2 else left_row(j, c)
            return pl.ds(pl.multiple_of(jnp.where(g < first, early, late), PIECE), PIECE)

        def out_copy(g, i):
            slot = g % 2
            return pltpu.make_async_copy(ho.at[slot, pl.ds(i * PIECE, PIECE)], h_ref.at[group_row(g, i)], ho_sem.at[slot, i])

        def wait_out(g):
            for i in range(per_group):
                out_copy(g, i).wait()

        def compute_qkv(g):
            slot = g % 2

            @pl.when(g >= own_groups)
            def _():
                for i in range(per_group):
                    lhs_copy(xg_ref.at[rows_at(me, i)], slot, i).wait()

            @pl.when(g >= 2)
            def _():
                wait_out(g - 2)

            tile = jnp.dot(lhs[slot], wq_v[...], preferred_element_type=f32).astype(bf16)
            for i in range(per_group):
                qkv_v[group_row(g, i), :] = tile[i * PIECE:(i + 1) * PIECE]

        def compute_up(g):
            slot = g % 2
            pre = lax.dot_general(lhs[slot], w1_v[...], (((1,), (1,)), ((), ())), preferred_element_type=f32)
            ho[slot] = jax.nn.gelu(pre, approximate=True).astype(bf16)
            for i in range(per_group):
                out_copy(g, i).start()

        def step(g):
            ahead = g < groups - LATE

            @pl.when(ahead)
            def _():
                fetch_links(g + 1)

            compute_qkv(g)

            @pl.when(ahead)
            def _():
                fetch_partner(g + 1)

            compute_up(g)

            @pl.when(jnp.logical_not(ahead) & (g < groups - 1))
            def _():
                fetch_links(g + 1)
                fetch_partner(g + 1)

        each(groups, step)
        wait_out(jnp.int32(groups - 2))
        wait_out(jnp.int32(groups - 1))

        own_to_partner().wait_send()

        def finish_own(j):
            to_right(j).wait_send()
            to_left(j).wait_send()

        def finish_relay(j):
            relay(j, 0).wait_send()
            relay(j, 1).wait_send()

        def finish_share(j):
            share(j, 0, core).wait_send()
            share(j, 1, core).wait_send()

        each(own_pieces, finish_own)
        each(half, finish_relay)
        each(arrivals, finish_share)

    def attend_phase(s_v, o_v, h_v, acc, stage, x_v, y_v):
        head_dim = qkv_head // 3
        tokens = qkv_v.shape[0]
        firsts = chunk // FIRST
        blocks = chunk // BLOCK
        half = width // 2
        slices = BLOCK // PIECE
        factor = head_dim ** -0.5 * math.log2(math.e)

        def block_rows(i, size):
            return pl.ds(pl.multiple_of(i * size, size), size)

        def to_partner(p, i, size, side):
            cols = pl.ds(side * half, half)
            src = acc.at[0, pl.ds(0, size), cols]
            dst = rp_ref.at[block_rows(i, size), cols]
            return remote(src, dst, send_p.at[p, side], recv_p.at[p, side], partner)

        def to_side(b, side):
            src = ps_ref.at[block_rows(b, FIRST), pl.ds(side * half, half)]
            dst = ro_ref.at[block_rows(side * firsts + b, FIRST)]
            return remote(src, dst, send_o.at[side, b], recv_o.at[side, b], left if side else right)

        def to_owner(q, k):
            side, block = q % 2, q // 2
            i = block * slices + k
            src = ps_ref.at[block_rows(firsts * FIRST // PIECE + q * slices + k, PIECE)]
            dst = rn_ref.at[block_rows(side * blocks * slices + i, PIECE)]
            device = (chip + 1 + 2 * side) % chips * CORES + core
            return remote(src, dst, send_n.at[side, i], recv_n.at[side, i], device)

        def attend_head(size, row, head):
            base = pl.multiple_of(head * qkv_head, head_dim)
            q = qkv_v[row, pl.ds(base, head_dim)]
            k_cols = pl.ds(pl.multiple_of(base + head_dim, head_dim), head_dim)
            v_cols = pl.ds(pl.multiple_of(base + 2 * head_dim, head_dim), head_dim)
            s = lax.dot_general(q, qkv_v[:, k_cols], (((1,), (1,)), ((), ())), preferred_element_type=f32)
            s_v[pl.ds(0, size), :] = s
            top = jnp.max(s, axis=-1, keepdims=True)
            e = jnp.exp2((s_v[pl.ds(0, size), :] - top) * factor)
            total = jnp.sum(e, axis=-1, keepdims=True)
            out = jnp.dot(e.astype(bf16), qkv_v[:, v_cols], preferred_element_type=f32)
            o_v[pl.ds(0, size), pl.ds(pl.multiple_of(head * head_dim, head_dim), head_dim)] = (out / total).astype(bf16)

        def partial(size, device, block, mine, between, after):
            row = block_rows(device * (chunk // size) + block, size)
            part = pl.ds(0, size)
            load_h = pltpu.make_async_copy(h_ref.at[row], h_v.at[part], h_sem)
            load_h.start()
            each(heads, lambda head: attend_head(size, row, head))
            load_h.wait()
            between()
            for n in range(width // COLS):
                cols = pl.ds(n * COLS, COLS)
                acc[mine, part, cols] = jnp.dot(
                    o_v[part, :], wo_v[:, cols], preferred_element_type=f32
                ) + jnp.dot(h_v[part, :], w2_v[:, cols], preferred_element_type=f32)
                after(n)

        def stage_partner(i, size):
            return pltpu.make_async_copy(rp_ref.at[block_rows(i, size)], stage.at[0, pl.ds(0, size)], st_sem.at[0])

        def stage_side(side, block):
            src = ro_ref.at[block_rows(side * blocks + block, BLOCK)]
            return pltpu.make_async_copy(src, stage.at[1, :, pl.ds(0, half)], st_sem.at[1])

        def add(size, base, slot, count):
            def tile(n):
                dst = pl.ds(pl.multiple_of(base + n * LANES, LANES), LANES)
                src = pl.ds(pl.multiple_of(n * LANES, LANES), LANES)
                acc[1, pl.ds(0, size), dst] += stage[slot, pl.ds(0, size), src]

            each(count // LANES, tile)

        def spill(i, size):
            return pltpu.make_async_copy(acc.at[1, pl.ds(0, size)], ps_ref.at[block_rows(i, size)], ps_sem)

        def collect(p, i, size):
            to_partner(p, i, size, 0).wait_recv()
            to_partner(p, i, size, 1).wait_recv()
            stage_partner(i, size).start()

        def halves_sent(p, i, size):
            to_partner(p, i, size, 0).wait_send()
            to_partner(p, i, size, 1).wait_send()

        def first_step(s):
            p = s // 2
            mine = jnp.where(p == 0, 1 - (s + core) % 2, s % 2)
            device = (chip + 2) % chips * CORES + (core + 1 - mine) % 2

            def between():
                @pl.when(s == 0)
                def _():
                    load_wo.wait()
                    load_w2.wait()

                @pl.when((mine == 0) & (p > 0))
                def _():
                    halves_sent(p - 1, p - 1, FIRST)

                @pl.when((mine == 1) & (p > 0))
                def _():
                    collect(p, p, FIRST)

            def after(n):
                @pl.when(mine == 0)
                def _():
                    to_partner(p, p, FIRST, n).start()

            partial(FIRST, device, p, mine, between, after)

            @pl.when(mine == 1)
            def _():
                @pl.when(p == 0)
                def _():
                    collect(p, p, FIRST)

                stage_partner(p, FIRST).wait()
                add(FIRST, 0, 0, width)
                spill(p, FIRST).start()
                spill(p, FIRST).wait()
                to_side(p, 0).start()
                to_side(p, 1).start()

        def later_step(s):
            q = s // 2
            mine = s % 2
            is_mid = q < 2 * blocks
            side = q % 2
            offset = jnp.where(is_mid, 1 + 2 * side, 0)
            block = jnp.where(is_mid, q // 2, q - 2 * blocks)
            device = (chip + offset) % chips * CORES + (core + 1 - mine) % 2
            p = firsts + q
            place = firsts * FIRST // BLOCK + q

            def between():
                @pl.when((mine == 0) & (q == 0))
                def _():
                    halves_sent(firsts - 1, firsts - 1, FIRST)

                @pl.when((mine == 0) & (q > 0))
                def _():
                    halves_sent(p - 1, place - 1, BLOCK)

                @pl.when(mine == 1)
                def _():
                    collect(p, place, BLOCK)

                    @pl.when(is_mid)
                    def _():
                        for k in range(BLOCK // FIRST):
                            b = block * (BLOCK // FIRST) + k
                            part = ro_ref.at[block_rows(side * firsts + b, FIRST)]
                            remote(part, part, recv_o.at[side, b], recv_o.at[side, b], partner).wait_recv()
                        stage_side(side, block).start()

            def after(n):
                @pl.when(mine == 0)
                def _():
                    to_partner(p, place, BLOCK, n).start()

            partial(BLOCK, device, block, mine, between, after)

            @pl.when(mine == 1)
            def _():
                stage_partner(place, BLOCK).wait()
                add(BLOCK, 0, 0, width)

                @pl.when(is_mid)
                def _():
                    stage_side(side, block).wait()
                    add(BLOCK, side * half, 1, half)
                    spill(place, BLOCK).start()
                    spill(place, BLOCK).wait()
                    each(slices, lambda k: to_owner(q, k).start())

                @pl.when(jnp.logical_not(is_mid))
                def _():
                    def final(k):
                        i = block * slices + k
                        rows = block_rows(i, PIECE)
                        load_x = pltpu.make_async_copy(x_ref.at[rows], x_v, xr_sem)
                        load_x.start()
                        copies = []
                        for sd in range(2):
                            src, sem = rn_ref.at[block_rows(sd * blocks * slices + i, PIECE)], recv_n.at[sd, i]
                            remote(src, src, sem, sem, partner).wait_recv()
                            copy = pltpu.make_async_copy(src, stage.at[sd, pl.ds(0, PIECE)], st_sem.at[sd])
                            copy.start()
                            copies.append(copy)
                        load_x.wait()
                        for copy in copies:
                            copy.wait()

                        def finish(n):
                            cols = pl.ds(pl.multiple_of(n * LANES, LANES), LANES)
                            part = pl.ds(0, PIECE)
                            summed = acc[1, block_rows(k, PIECE), cols] + stage[0, part, cols] + stage[1, part, cols]
                            y_v[:, cols] = (x_v[:, cols].astype(f32) + summed).astype(bf16)

                        each(width // LANES, finish)
                        store = pltpu.make_async_copy(y_v, y_ref.at[rows], y_sem)
                        store.start()
                        store.wait()

                    each(slices, final)

        each(2 * firsts, first_step)
        each(2 * blocks * (chips - 1), later_step)
        last = blocks * (chips - 1) - 1
        halves_sent(firsts + last, firsts * FIRST // BLOCK + last, BLOCK)

        def finish_side(b):
            to_side(b, 0).wait_send()
            to_side(b, 1).wait_send()

        each(firsts, finish_side)
        each(2 * blocks, lambda q: each(slices, lambda k: to_owner(q, k).wait_send()))

    ff_width = w1_ref.shape[0]
    pl.run_scoped(
        project_phase,
        pltpu.VMEM((width, heads * qkv_head), bf16),
        pltpu.VMEM(w1_ref.shape, bf16),
        pltpu.VMEM((2, REPACK, heads, qkv_head), bf16),
        pltpu.VMEM((2, GROUP, width), bf16),
        pltpu.VMEM((2, GROUP, ff_width), bf16),
    )
    pl.run_scoped(
        attend_phase,
        pltpu.VMEM((BLOCK, qkv_v.shape[0]), f32),
        pltpu.VMEM((BLOCK, wo_v.shape[0]), bf16),
        pltpu.VMEM((BLOCK, ff_width), bf16),
        pltpu.VMEM((2, BLOCK, width), f32),
        pltpu.VMEM((2, BLOCK, width), f32),
        pltpu.VMEM((PIECE, width), bf16),
        pltpu.VMEM((PIECE, width), bf16),
    )


def transformer_block(chips, x_loc, ln_gamma, w_qkv, w_out, w_up_t, w_down):
    chunk, width = x_loc.shape
    tokens = chunk * chips * CORES
    heads, qkv_head = w_qkv.shape[1], w_qkv.shape[2]
    ff_width = w_up_t.shape[0]
    arrivals = chunk // PIECE + chunk // PIECE // 2
    firsts = chunk // FIRST
    pieces = chunk // PIECE
    pairs = firsts + (chips - 1) * (chunk // BLOCK)
    per_group = GROUP // PIECE
    bf16, f32 = jnp.bfloat16, jnp.float32
    dma = pltpu.SemaphoreType.DMA
    out = pl.pallas_call(
        functools.partial(block_kernel, chips),
        in_specs=[ANY] * 6,
        out_specs=[ANY] * 7,
        out_shape=[
            jax.ShapeDtypeStruct((chunk, width), bf16),
            jax.ShapeDtypeStruct((tokens, width), bf16),
            jax.ShapeDtypeStruct((tokens, ff_width), bf16),
            jax.ShapeDtypeStruct((chips * chunk, width), f32),
            jax.ShapeDtypeStruct((2 * chunk, width // 2), f32),
            jax.ShapeDtypeStruct((2 * chunk, width), f32),
            jax.ShapeDtypeStruct((3 * chunk, width), f32),
        ],
        scratch_shapes=[
            pltpu.VMEM((tokens, heads * qkv_head), bf16),
            pltpu.VMEM(w_out.shape, bf16),
            pltpu.VMEM(w_down.shape, bf16),
            pltpu.VMEM((1, width), f32),
            dma((4,)), dma((chunk // GROUP,)), dma((2,)), dma((2, per_group)), dma((2, per_group)),
            dma((arrivals,)), dma((arrivals,)), dma((arrivals,)), dma((arrivals,)),
            dma((2 * arrivals + 1,)), dma((2 * arrivals + 1,)),
            dma, dma((2,)), dma, dma, dma,
            dma((pairs, 2)), dma((pairs, 2)),
            dma((2, firsts)), dma((2, firsts)),
            dma((2, pieces)), dma((2, pieces)),
        ],
        compiler_params=pltpu.CompilerParams(collective_id=0, has_side_effects=True, vmem_limit_bytes=VMEM_LIMIT),
        name="transformer_block",
    )(x_loc, ln_gamma.reshape(1, width), w_qkv, w_out, w_up_t, w_down)
    return out[0]


def solution(mesh):
    chips = mesh.shape["tp"] // CORES

    def local_block(x_loc, ln_gamma, w_qkv, w_out, w_up, w_down):
        heads, head_dim, model_dim = w_out.shape
        return transformer_block(chips, x_loc, ln_gamma, w_qkv, w_out.reshape(heads * head_dim, model_dim), w_up.T, w_down)

    row_spec = P(("data", "tp"), None)
    return jax.shard_map(local_block, mesh=mesh, in_specs=(row_spec, P(None), P(None, "tp", None), P("tp", None, None), P(None, "tp"), P("tp", None)), out_specs=row_spec, check_vma=False)
```

```python
import functools
import math

import jax
import jax.numpy as jnp
from jax import lax
from jax.experimental import pallas as pl
from jax.experimental.pallas import tpu as pltpu
from jax.sharding import PartitionSpec as P

LN_EPS = 1e-6
MESH = pl.DeviceIdType.MESH
CORES = 2
PIECE = 64
GROUP = 256
BLOCK = 128
FIRST = 64
HELD = 2
REPACK = 256
LATE = 3
COLS = 2048
LANES = 512
VMEM_LIMIT = 67_000_000
ANY = pl.BlockSpec(memory_space=pl.ANY)


def neighbours(chips):
    me = lax.axis_index("tp")
    chip, core = me // CORES, me % CORES
    right = (chip + 1) % chips * CORES + core
    left = (chip + chips - 1) % chips * CORES + core
    partner = chip * CORES + (1 - core)
    return me, chip, core, right, left, partner


def greet(devices):
    barrier = pltpu.get_barrier_semaphore()
    for device in devices:
        pl.semaphore_signal(barrier, inc=1, device_id={"tp": device}, device_id_type=MESH)
    pl.semaphore_wait(barrier, len(devices))


def remote(src, dst, send_sem, recv_sem, device):
    return pltpu.make_async_remote_copy(
        src_ref=src, dst_ref=dst, send_sem=send_sem, recv_sem=recv_sem, device_id={"tp": device}, device_id_type=MESH
    )


def each(count, body):
    def step(i, carry):
        body(i)
        return carry

    lax.fori_loop(0, count, step, 0)


def block_kernel(
    chips, x_ref, gamma_ref, wq_ref, wo_ref, w1_ref, w2_ref,
    y_ref, xg_ref, h_ref, rp_ref, ro_ref, rn_ref, ps_ref,
    qkv_v, wo_v, w2_v, w1_v, lhs, ho, gamma_v,
    w_sem, x_sem, wq_sem, lhs_sem, ho_sem, send_r, recv_l, send_l, recv_r, send_g, recv_g,
    h_sem, st_sem, xr_sem, y_sem, ps_sem, send_p, recv_p, send_o, recv_o, send_n, recv_n,
):
    me, chip, core, right, left, partner = neighbours(chips)
    chunk, width = x_ref.shape
    heads, qkv_head = wq_ref.shape[1], wq_ref.shape[2]
    load_wo = pltpu.make_async_copy(wo_ref, wo_v, w_sem.at[1])
    load_w2 = pltpu.make_async_copy(w2_ref, w2_v, w_sem.at[2])
    bf16, f32 = jnp.bfloat16, jnp.float32

    own_pieces = chunk // PIECE
    half = own_pieces // 2
    arrivals = own_pieces + half
    per_group = GROUP // PIECE
    own_groups = chunk // GROUP
    first = own_groups * CORES
    groups = first + arrivals

    def load_x(piece):
        slot, row = piece // per_group, piece % per_group * PIECE
        return pltpu.make_async_copy(x_ref.at[pl.ds(piece * PIECE, PIECE)], lhs.at[slot, pl.ds(row, PIECE)], x_sem.at[piece])

    for j in range(half):
        load_x(j).start()
        load_x(j + half).start()
    load_gamma = pltpu.make_async_copy(gamma_ref, gamma_v, w_sem.at[3])
    load_gamma.start()

    load_w1 = pltpu.make_async_copy(w1_ref, w1_v, w_sem.at[0])
    greet((right, left, partner))

    def rows_at(device, piece):
        return pl.ds(pl.multiple_of(device * chunk + piece * PIECE, PIECE), PIECE)

    def own_send(piece, sends, recvs, j, device):
        rows = xg_ref.at[rows_at(me, piece)]
        return remote(rows, rows, sends.at[j], recvs.at[j], device)

    def to_right(j):
        return own_send(j, send_r, recv_l, j, right)

    def to_left(j):
        return own_send((j + half) % own_pieces, send_l, recv_r, j, left)

    def own_to_partner():
        rows = xg_ref.at[pl.ds(pl.multiple_of(me * chunk, chunk), chunk)]
        return remote(rows, rows, send_g.at[2 * arrivals], recv_g.at[2 * arrivals], partner)

    def normalise(j):
        out = []
        for side in range(2):
            rows = pl.ds(j * PIECE, PIECE)
            piece = j + side * half
            load_x(piece).wait()
            vals = lhs[side, rows, :].astype(f32)
            centered = vals - jnp.mean(vals, axis=-1, keepdims=True)
            var = jnp.mean(centered * centered, axis=-1, keepdims=True)
            lhs[side, rows, :] = (centered * lax.rsqrt(var + LN_EPS) * gamma_v[...]).astype(bf16)
            copy = pltpu.make_async_copy(lhs.at[side, rows], xg_ref.at[rows_at(me, piece)], lhs_sem.at[side, 0])
            copy.start()
            out.append(copy)
        for copy in out:
            copy.wait()

    def left_row(j, c):
        return ((chip + chips - 1 - j // own_pieces) % chips * CORES + c) * chunk + j % own_pieces * PIECE

    def right_row(j, c):
        return ((chip + 1 + j // own_pieces) % chips * CORES + c) * chunk + (j + half) % own_pieces * PIECE

    def side_rows(j, side, c):
        row = right_row(j, c) if side else left_row(j, c)
        return pl.ds(pl.multiple_of(row, PIECE), PIECE)

    def lhs_copy(src, slot, i):
        return pltpu.make_async_copy(src, lhs.at[slot, pl.ds(i * PIECE, PIECE)], lhs_sem.at[slot, i])

    def relay(j, side):
        rows = xg_ref.at[side_rows(j, side, core)]
        sends, recvs, device = (send_l, recv_r, left) if side else (send_r, recv_l, right)
        return remote(rows, rows, sends.at[own_pieces + j], recvs.at[own_pieces + j], device)

    def share(j, side, c):
        rows = xg_ref.at[side_rows(j, side, c)]
        return remote(rows, rows, send_g.at[2 * j + side], recv_g.at[2 * j + side], partner)

    def fetch_links(g):
        slot = g % 2

        @pl.when((g >= own_groups) & (g < first))
        def _():
            @pl.when(g == own_groups)
            def _():
                own_to_partner().wait_recv()

            for i in range(per_group):
                lhs_copy(xg_ref.at[rows_at(partner, (g - own_groups) * per_group + i)], slot, i).start()

        @pl.when(g >= first)
        def _():
            j = g - first
            for side in range(2):
                rows = xg_ref.at[side_rows(j, side, core)]
                sem = (recv_r if side else recv_l).at[j]
                remote(rows, rows, sem, sem, partner).wait_recv()

            @pl.when(j < half)
            def _():
                relay(j, 0).start()
                relay(j, 1).start()

            for side in range(2):
                share(j, side, core).start()
                lhs_copy(xg_ref.at[side_rows(j, side, core)], slot, side).start()

    def fetch_partner(g):
        @pl.when(g >= first)
        def _():
            j = g - first
            for side in range(2):
                share(j, side, 1 - core).wait_recv()
            for side in range(2):
                lhs_copy(xg_ref.at[side_rows(j, side, 1 - core)], g % 2, 2 + side).start()

    def group_row(g, i):
        j = g - first
        early = jnp.where(g < own_groups, me, partner) * chunk + ((g % own_groups) * per_group + i) * PIECE
        c = core if i < 2 else 1 - core
        late = right_row(j, c) if i % 2 else left_row(j, c)
        return pl.ds(pl.multiple_of(jnp.where(g < first, early, late), PIECE), PIECE)

    def out_copy(g, i):
        slot = g % 2
        return pltpu.make_async_copy(ho.at[slot, pl.ds(i * PIECE, PIECE)], h_ref.at[group_row(g, i)], ho_sem.at[slot, i])

    def wait_out(g):
        for i in range(per_group):
            out_copy(g, i).wait()

    def compute_up(g):
        slot = g % 2

        @pl.when((g >= 2) & (g < groups - HELD))
        def _():
            wait_out(g - 2)

        pre = lax.dot_general(lhs[slot], w1_v[...], (((1,), (1,)), ((), ())), preferred_element_type=f32)
        ho[slot] = jax.nn.gelu(pre, approximate=True).astype(bf16)
        for i in range(per_group):
            out_copy(g, i).start()

    def finish_gather():
        own_to_partner().wait_send()

        def finish_own(j):
            to_right(j).wait_send()
            to_left(j).wait_send()

        def finish_relay(j):
            relay(j, 0).wait_send()
            relay(j, 1).wait_send()

        def finish_share(j):
            share(j, 0, core).wait_send()
            share(j, 1, core).wait_send()

        each(own_pieces, finish_own)
        each(half, finish_relay)
        each(arrivals, finish_share)

    def project_phase(wq_v, w4_v):
        def load_wq(i):
            rows = pl.ds(pl.multiple_of(i * REPACK, REPACK), REPACK)
            return pltpu.make_async_copy(wq_ref.at[rows], w4_v.at[i % 2], wq_sem.at[i % 2])

        load_wq(0).start()
        load_w1.start()
        load_gamma.wait()
        for j in range(half):
            normalise(j)
            to_right(j).start()
            to_left(j).start()
        own_to_partner().start()

        def open_rest(j):
            to_right(half + j).start()
            to_left(half + j).start()

        each(half, open_rest)
        load_wo.start()
        load_w2.start()

        def repack(i):
            @pl.when(i < width // REPACK - 1)
            def _():
                load_wq(i + 1).start()

            load_wq(i).wait()
            rows = pl.ds(pl.multiple_of(i * REPACK, REPACK), REPACK)
            wq_v[rows, :] = w4_v[i % 2].reshape(REPACK, heads * qkv_head)

        each(width // REPACK, repack)
        load_w1.wait()

        def compute_qkv(g):
            slot = g % 2

            @pl.when(g >= own_groups)
            def _():
                for i in range(per_group):
                    lhs_copy(xg_ref.at[rows_at(me, i)], slot, i).wait()

            tile = jnp.dot(lhs[slot], wq_v[...], preferred_element_type=f32).astype(bf16)
            for i in range(per_group):
                qkv_v[group_row(g, i), :] = tile[i * PIECE:(i + 1) * PIECE]

        def step(g):
            ahead = g < groups - LATE

            @pl.when(ahead)
            def _():
                fetch_links(g + 1)

            compute_qkv(g)

            @pl.when(ahead)
            def _():
                fetch_partner(g + 1)

            @pl.when(g < groups - HELD)
            def _():
                compute_up(g)

            @pl.when(jnp.logical_not(ahead) & (g < groups - 1))
            def _():
                fetch_links(g + 1)
                fetch_partner(g + 1)

        each(groups, step)
        for g in range(groups - HELD - 2, groups - HELD):
            wait_out(jnp.int32(g))

    def attend_phase(s_v, o_v, h_v, away, acc, stage, stage_half, x_v, y_v):
        head_dim = qkv_head // 3
        firsts = chunk // FIRST
        blocks = chunk // BLOCK
        cols_half = width // 2
        slices = BLOCK // PIECE
        factor = head_dim ** -0.5 * math.log2(math.e)

        def block_rows(i, size):
            return pl.ds(pl.multiple_of(i * size, size), size)

        def to_partner(p, i, size, side):
            cols = pl.ds(side * cols_half, cols_half)
            src = away.at[pl.ds(0, size), cols]
            dst = rp_ref.at[block_rows(i, size), cols]
            return remote(src, dst, send_p.at[p, side], recv_p.at[p, side], partner)

        def to_side(b, side):
            src = ps_ref.at[block_rows(b, FIRST), pl.ds(side * cols_half, cols_half)]
            dst = ro_ref.at[block_rows(side * firsts + b, FIRST)]
            return remote(src, dst, send_o.at[side, b], recv_o.at[side, b], left if side else right)

        def to_owner(q, k):
            side, block = q % 2, q // 2
            i = block * slices + k
            src = ps_ref.at[block_rows(firsts * FIRST // PIECE + q * slices + k, PIECE)]
            dst = rn_ref.at[block_rows(side * blocks * slices + i, PIECE)]
            device = (chip + 1 + 2 * side) % chips * CORES + core
            return remote(src, dst, send_n.at[side, i], recv_n.at[side, i], device)

        def attend_head(size, rows, head):
            base = pl.multiple_of(head * qkv_head, head_dim)
            q = jnp.concatenate([qkv_v[row, pl.ds(base, head_dim)] for row in rows], axis=0)
            k_cols = pl.ds(pl.multiple_of(base + head_dim, head_dim), head_dim)
            v_cols = pl.ds(pl.multiple_of(base + 2 * head_dim, head_dim), head_dim)
            part = pl.ds(0, 2 * size)
            s = lax.dot_general(q, qkv_v[:, k_cols], (((1,), (1,)), ((), ())), preferred_element_type=f32)
            s_v[part, :] = s
            top = jnp.max(s, axis=-1, keepdims=True)
            e = jnp.exp2((s_v[part, :] - top) * factor)
            total = jnp.sum(e, axis=-1, keepdims=True)
            out = jnp.dot(e.astype(bf16), qkv_v[:, v_cols], preferred_element_type=f32)
            o_v[part, pl.ds(pl.multiple_of(head * head_dim, head_dim), head_dim)] = (out / total).astype(bf16)

        def stage_partner(i, size):
            return pltpu.make_async_copy(rp_ref.at[block_rows(i, size)], stage.at[pl.ds(0, size)], st_sem.at[0])

        def stage_side(side, block):
            src = ro_ref.at[block_rows(side * blocks + block, BLOCK)]
            return pltpu.make_async_copy(src, stage_half, st_sem.at[1])

        def add(size, slot, base, addend):
            def tile(n):
                dst = pl.ds(pl.multiple_of(base + n * LANES, LANES), LANES)
                src = pl.ds(pl.multiple_of(n * LANES, LANES), LANES)
                acc[slot, pl.ds(0, size), dst] += addend[pl.ds(0, size), src]

            each(addend.shape[1] // LANES, tile)

        def spill(slot, i, size):
            return pltpu.make_async_copy(acc.at[slot, pl.ds(0, size)], ps_ref.at[block_rows(i, size)], ps_sem)

        def collect(p, i, size):
            to_partner(p, i, size, 0).wait_recv()
            to_partner(p, i, size, 1).wait_recv()
            stage_partner(i, size).start()

        def sent(p, i, size):
            to_partner(p, i, size, 0).wait_send()
            to_partner(p, i, size, 1).wait_send()

        def partial(size, p, i, chip_offset, block, between):
            base = (chip + chip_offset) % chips * CORES
            rows = [block_rows((base + c) * (chunk // size) + block, size) for c in (1 - core, core)]
            loads = [
                pltpu.make_async_copy(h_ref.at[row], h_v.at[pl.ds(n * size, size)], h_sem.at[n])
                for n, row in enumerate(rows)
            ]
            for load in loads:
                load.start()
            each(heads, lambda head: attend_head(size, rows, head))
            for load in loads:
                load.wait()
            between()
            part = pl.ds(0, 2 * size)
            for n in range(width // COLS):
                cols = pl.ds(n * COLS, COLS)
                both = jnp.dot(
                    o_v[part, :], wo_v[:, cols], preferred_element_type=f32
                ) + jnp.dot(h_v[part, :], w2_v[:, cols], preferred_element_type=f32)
                away[pl.ds(0, size), cols] = both[:size]
                acc[p % 2, pl.ds(0, size), cols] = both[size:]
                to_partner(p, i, size, n).start()

        def first_collect(s):
            collect(s, s, FIRST)

        def first_finish(s):
            slot = s % 2
            stage_partner(s, FIRST).wait()
            add(FIRST, slot, 0, stage)
            spill(slot, s, FIRST).start()
            spill(slot, s, FIRST).wait()
            to_side(s, 0).start()
            to_side(s, 1).start()

        def first_step(s):
            def between():
                @pl.when(s == 0)
                def _():
                    load_wo.wait()
                    load_w2.wait()

                @pl.when(s > 0)
                def _():
                    sent(s - 1, s - 1, FIRST)

                @pl.when(s > HELD)
                def _():
                    first_collect(s - 1)

            partial(FIRST, s, s, 2, s, between)

            @pl.when(s < HELD)
            def _():
                compute_up(groups - HELD + s)
                first_collect(s)
                first_finish(s)

            @pl.when(s == HELD - 1)
            def _():
                for g in range(groups - HELD, groups):
                    wait_out(jnp.int32(g))

            @pl.when(s > HELD)
            def _():
                first_finish(s - 1)

        skip = firsts * FIRST // BLOCK

        def later_parts(q):
            is_mid = q < 2 * blocks
            return is_mid, q % 2, jnp.where(is_mid, q // 2, q - 2 * blocks)

        def later_collect(q):
            is_mid, side, block = later_parts(q)
            collect(firsts + q, skip + q, BLOCK)

            @pl.when(is_mid)
            def _():
                for k in range(BLOCK // FIRST):
                    b = block * (BLOCK // FIRST) + k
                    part = ro_ref.at[block_rows(side * firsts + b, FIRST)]
                    remote(part, part, recv_o.at[side, b], recv_o.at[side, b], partner).wait_recv()
                stage_side(side, block).start()

        def later_finish(q):
            is_mid, side, block = later_parts(q)
            slot = (firsts + q) % 2
            stage_partner(skip + q, BLOCK).wait()
            add(BLOCK, slot, 0, stage)

            @pl.when(is_mid)
            def _():
                stage_side(side, block).wait()
                add(BLOCK, slot, side * cols_half, stage_half)
                spill(slot, skip + q, BLOCK).start()
                spill(slot, skip + q, BLOCK).wait()
                each(slices, lambda k: to_owner(q, k).start())

            @pl.when(jnp.logical_not(is_mid))
            def _():
                def final(k):
                    i = block * slices + k
                    rows = block_rows(i, PIECE)
                    load = pltpu.make_async_copy(x_ref.at[rows], x_v, xr_sem)
                    load.start()
                    copies = []
                    for sd in range(2):
                        src, sem = rn_ref.at[block_rows(sd * blocks * slices + i, PIECE)], recv_n.at[sd, i]
                        remote(src, src, sem, sem, partner).wait_recv()
                        copy = pltpu.make_async_copy(src, stage.at[pl.ds(sd * PIECE, PIECE)], st_sem.at[sd])
                        copy.start()
                        copies.append(copy)
                    load.wait()
                    for copy in copies:
                        copy.wait()

                    def tile(n):
                        cols = pl.ds(pl.multiple_of(n * LANES, LANES), LANES)
                        mine = acc[slot, block_rows(k, PIECE), cols]
                        summed = mine + stage[0:PIECE, cols] + stage[PIECE:2 * PIECE, cols]
                        y_v[:, cols] = (x_v[:, cols].astype(f32) + summed).astype(bf16)

                    each(width // LANES, tile)
                    store = pltpu.make_async_copy(y_v, y_ref.at[rows], y_sem)
                    store.start()
                    store.wait()

                each(slices, final)

        def later_step(q):
            is_mid, side, block = later_parts(q)
            p = firsts + q

            def between():
                @pl.when(q == 0)
                def _():
                    sent(firsts - 1, firsts - 1, FIRST)

                @pl.when(q > 0)
                def _():
                    sent(p - 1, skip + q - 1, BLOCK)
                    later_collect(q - 1)

            partial(BLOCK, p, skip + q, jnp.where(is_mid, 1 + 2 * side, 0), block, between)

            @pl.when(q > 0)
            def _():
                later_finish(q - 1)

        later = blocks * (chips - 1)
        each(firsts, first_step)
        first_collect(jnp.int32(firsts - 1))
        first_finish(jnp.int32(firsts - 1))
        each(later, later_step)
        later_collect(jnp.int32(later - 1))
        later_finish(jnp.int32(later - 1))
        sent(jnp.int32(firsts + later - 1), jnp.int32(skip + later - 1), BLOCK)

        def finish_side(b):
            to_side(b, 0).wait_send()
            to_side(b, 1).wait_send()

        each(firsts, finish_side)
        each(2 * blocks, lambda q: each(slices, lambda k: to_owner(q, k).wait_send()))

    pl.run_scoped(
        project_phase,
        pltpu.VMEM((width, heads * qkv_head), bf16),
        pltpu.VMEM((2, REPACK, heads, qkv_head), bf16),
    )
    pl.run_scoped(
        attend_phase,
        pltpu.VMEM((2 * BLOCK, qkv_v.shape[0]), f32),
        pltpu.VMEM((2 * BLOCK, wo_v.shape[0]), bf16),
        pltpu.VMEM((2 * BLOCK, h_ref.shape[1]), bf16),
        pltpu.VMEM((BLOCK, width), f32),
        pltpu.VMEM((2, BLOCK, width), f32),
        pltpu.VMEM((BLOCK, width), f32),
        pltpu.VMEM((BLOCK, width // 2), f32),
        pltpu.VMEM((PIECE, width), bf16),
        pltpu.VMEM((PIECE, width), bf16),
    )
    finish_gather()


def transformer_block(chips, x_loc, ln_gamma, w_qkv, w_out, w_up_t, w_down):
    chunk, width = x_loc.shape
    tokens = chunk * chips * CORES
    heads, qkv_head = w_qkv.shape[1], w_qkv.shape[2]
    ff_width = w_up_t.shape[0]
    arrivals = chunk // PIECE + chunk // PIECE // 2
    firsts = chunk // FIRST
    pieces = chunk // PIECE
    pairs = firsts + (chips - 1) * (chunk // BLOCK)
    per_group = GROUP // PIECE
    bf16, f32 = jnp.bfloat16, jnp.float32
    dma = pltpu.SemaphoreType.DMA
    out = pl.pallas_call(
        functools.partial(block_kernel, chips),
        in_specs=[ANY] * 6,
        out_specs=[ANY] * 7,
        out_shape=[
            jax.ShapeDtypeStruct((chunk, width), bf16),
            jax.ShapeDtypeStruct((tokens, width), bf16),
            jax.ShapeDtypeStruct((tokens, ff_width), bf16),
            jax.ShapeDtypeStruct((chips * chunk, width), f32),
            jax.ShapeDtypeStruct((2 * chunk, width // 2), f32),
            jax.ShapeDtypeStruct((2 * chunk, width), f32),
            jax.ShapeDtypeStruct((3 * chunk, width), f32),
        ],
        scratch_shapes=[
            pltpu.VMEM((tokens, heads * qkv_head), bf16),
            pltpu.VMEM(w_out.shape, bf16),
            pltpu.VMEM(w_down.shape, bf16),
            pltpu.VMEM(w_up_t.shape, bf16),
            pltpu.VMEM((2, GROUP, width), bf16),
            pltpu.VMEM((2, GROUP, ff_width), bf16),
            pltpu.VMEM((1, width), f32),
            dma((4,)), dma((pieces,)), dma((2,)), dma((2, per_group)), dma((2, per_group)),
            dma((arrivals,)), dma((arrivals,)), dma((arrivals,)), dma((arrivals,)),
            dma((2 * arrivals + 1,)), dma((2 * arrivals + 1,)),
            dma((2,)), dma((2,)), dma, dma, dma,
            dma((pairs, 2)), dma((pairs, 2)),
            dma((2, firsts)), dma((2, firsts)),
            dma((2, pieces)), dma((2, pieces)),
        ],
        compiler_params=pltpu.CompilerParams(collective_id=0, has_side_effects=True, vmem_limit_bytes=VMEM_LIMIT),
        name="transformer_block",
    )(x_loc, ln_gamma.reshape(1, width), w_qkv, w_out, w_up_t, w_down)
    return out[0]


def solution(mesh):
    chips = mesh.shape["tp"] // CORES

    def local_block(x_loc, ln_gamma, w_qkv, w_out, w_up, w_down):
        heads, head_dim, model_dim = w_out.shape
        return transformer_block(chips, x_loc, ln_gamma, w_qkv, w_out.reshape(heads * head_dim, model_dim), w_up.T, w_down)

    row_spec = P(("data", "tp"), None)
    return jax.shard_map(local_block, mesh=mesh, in_specs=(row_spec, P(None), P(None, "tp", None), P("tp", None, None), P(None, "tp"), P("tp", None)), out_specs=row_spec, check_vma=False)
```

```python
import functools
import math

import jax
import jax.numpy as jnp
from jax import lax
from jax.experimental import pallas as pl
from jax.experimental.pallas import tpu as pltpu
from jax.sharding import PartitionSpec as P

LN_EPS = 1e-6
MESH = pl.DeviceIdType.MESH
CORES = 2
PIECE = 64
GROUP = 256
BLOCK = 128
FIRST = 64
HELD = 1
REPACK = 256
LATE = 3
COLS = 2048
LANES = 512
VMEM_LIMIT = 67_000_000
ANY = pl.BlockSpec(memory_space=pl.ANY)


def neighbours(chips):
    me = lax.axis_index("tp")
    chip, core = me // CORES, me % CORES
    right = (chip + 1) % chips * CORES + core
    left = (chip + chips - 1) % chips * CORES + core
    partner = chip * CORES + (1 - core)
    return me, chip, core, right, left, partner


def greet(devices):
    barrier = pltpu.get_barrier_semaphore()
    for device in devices:
        pl.semaphore_signal(barrier, inc=1, device_id={"tp": device}, device_id_type=MESH)
    pl.semaphore_wait(barrier, len(devices))


def remote(src, dst, send_sem, recv_sem, device):
    return pltpu.make_async_remote_copy(
        src_ref=src, dst_ref=dst, send_sem=send_sem, recv_sem=recv_sem, device_id={"tp": device}, device_id_type=MESH
    )


def each(count, body):
    def step(i, carry):
        body(i)
        return carry

    lax.fori_loop(0, count, step, 0)


def block_kernel(
    chips, x_ref, gamma_ref, wq_ref, wo_ref, w1_ref, w2_ref,
    y_ref, xg_ref, h_ref, rp_ref, ro_ref, rn_ref, ps_ref,
    qkv_v, wo_v, w2_v, w1_v, lhs, ho, gamma_v,
    w_sem, x_sem, wq_sem, lhs_sem, ho_sem, send_r, recv_l, send_l, recv_r, send_g, recv_g,
    h_sem, st_sem, xr_sem, y_sem, ps_sem, send_p, recv_p, send_o, recv_o, send_n, recv_n,
):
    me, chip, core, right, left, partner = neighbours(chips)
    chunk, width = x_ref.shape
    heads, qkv_head = wq_ref.shape[1], wq_ref.shape[2]
    load_wo = pltpu.make_async_copy(wo_ref, wo_v, w_sem.at[1])
    load_w2 = pltpu.make_async_copy(w2_ref, w2_v, w_sem.at[2])
    bf16, f32 = jnp.bfloat16, jnp.float32

    own_pieces = chunk // PIECE
    half = own_pieces // 2
    arrivals = own_pieces + half
    per_group = GROUP // PIECE
    own_groups = chunk // GROUP
    first = own_groups * CORES
    groups = first + arrivals

    def load_x(piece):
        slot, row = piece // per_group, piece % per_group * PIECE
        return pltpu.make_async_copy(x_ref.at[pl.ds(piece * PIECE, PIECE)], lhs.at[slot, pl.ds(row, PIECE)], x_sem.at[piece])

    for j in range(half):
        load_x(j).start()
        load_x(j + half).start()
    load_gamma = pltpu.make_async_copy(gamma_ref, gamma_v, w_sem.at[3])
    load_gamma.start()

    load_w1 = pltpu.make_async_copy(w1_ref, w1_v, w_sem.at[0])
    greet((right, left, partner))

    def rows_at(device, piece):
        return pl.ds(pl.multiple_of(device * chunk + piece * PIECE, PIECE), PIECE)

    def own_send(piece, sends, recvs, j, device):
        rows = xg_ref.at[rows_at(me, piece)]
        return remote(rows, rows, sends.at[j], recvs.at[j], device)

    def to_right(j):
        return own_send(j, send_r, recv_l, j, right)

    def to_left(j):
        return own_send((j + half) % own_pieces, send_l, recv_r, j, left)

    def own_to_partner():
        rows = xg_ref.at[pl.ds(pl.multiple_of(me * chunk, chunk), chunk)]
        return remote(rows, rows, send_g.at[2 * arrivals], recv_g.at[2 * arrivals], partner)

    def normalise(j):
        out = []
        for side in range(2):
            rows = pl.ds(j * PIECE, PIECE)
            piece = j + side * half
            load_x(piece).wait()
            vals = lhs[side, rows, :].astype(f32)
            centered = vals - jnp.mean(vals, axis=-1, keepdims=True)
            var = jnp.mean(centered * centered, axis=-1, keepdims=True)
            lhs[side, rows, :] = (centered * lax.rsqrt(var + LN_EPS) * gamma_v[...]).astype(bf16)
            copy = pltpu.make_async_copy(lhs.at[side, rows], xg_ref.at[rows_at(me, piece)], lhs_sem.at[side, 0])
            copy.start()
            out.append(copy)
        for copy in out:
            copy.wait()

    def left_row(j, c):
        return ((chip + chips - 1 - j // own_pieces) % chips * CORES + c) * chunk + j % own_pieces * PIECE

    def right_row(j, c):
        return ((chip + 1 + j // own_pieces) % chips * CORES + c) * chunk + (j + half) % own_pieces * PIECE

    def side_rows(j, side, c):
        row = right_row(j, c) if side else left_row(j, c)
        return pl.ds(pl.multiple_of(row, PIECE), PIECE)

    def lhs_copy(src, slot, i):
        return pltpu.make_async_copy(src, lhs.at[slot, pl.ds(i * PIECE, PIECE)], lhs_sem.at[slot, i])

    def relay(j, side):
        rows = xg_ref.at[side_rows(j, side, core)]
        sends, recvs, device = (send_l, recv_r, left) if side else (send_r, recv_l, right)
        return remote(rows, rows, sends.at[own_pieces + j], recvs.at[own_pieces + j], device)

    def share(j, side, c):
        rows = xg_ref.at[side_rows(j, side, c)]
        return remote(rows, rows, send_g.at[2 * j + side], recv_g.at[2 * j + side], partner)

    def fetch_links(g):
        slot = g % 2

        @pl.when((g >= own_groups) & (g < first))
        def _():
            @pl.when(g == own_groups)
            def _():
                own_to_partner().wait_recv()

            for i in range(per_group):
                lhs_copy(xg_ref.at[rows_at(partner, (g - own_groups) * per_group + i)], slot, i).start()

        @pl.when(g >= first)
        def _():
            j = g - first
            for side in range(2):
                rows = xg_ref.at[side_rows(j, side, core)]
                sem = (recv_r if side else recv_l).at[j]
                remote(rows, rows, sem, sem, partner).wait_recv()

            @pl.when(j < half)
            def _():
                relay(j, 0).start()
                relay(j, 1).start()

            for side in range(2):
                share(j, side, core).start()
                lhs_copy(xg_ref.at[side_rows(j, side, core)], slot, side).start()

    def fetch_partner(g):
        @pl.when(g >= first)
        def _():
            j = g - first
            for side in range(2):
                share(j, side, 1 - core).wait_recv()
            for side in range(2):
                lhs_copy(xg_ref.at[side_rows(j, side, 1 - core)], g % 2, 2 + side).start()

    def group_row(g, i):
        j = g - first
        early = jnp.where(g < own_groups, me, partner) * chunk + ((g % own_groups) * per_group + i) * PIECE
        c = core if i < 2 else 1 - core
        late = right_row(j, c) if i % 2 else left_row(j, c)
        return pl.ds(pl.multiple_of(jnp.where(g < first, early, late), PIECE), PIECE)

    def out_copy(g, i):
        slot = g % 2
        return pltpu.make_async_copy(ho.at[slot, pl.ds(i * PIECE, PIECE)], h_ref.at[group_row(g, i)], ho_sem.at[slot, i])

    def wait_out(g):
        for i in range(per_group):
            out_copy(g, i).wait()

    def compute_up(g):
        slot = g % 2

        @pl.when((g >= 2) & (g < groups - HELD))
        def _():
            wait_out(g - 2)

        pre = lax.dot_general(lhs[slot], w1_v[...], (((1,), (1,)), ((), ())), preferred_element_type=f32)
        ho[slot] = jax.nn.gelu(pre, approximate=True).astype(bf16)
        for i in range(per_group):
            out_copy(g, i).start()

    def finish_gather():
        own_to_partner().wait_send()

        def finish_own(j):
            to_right(j).wait_send()
            to_left(j).wait_send()

        def finish_relay(j):
            relay(j, 0).wait_send()
            relay(j, 1).wait_send()

        def finish_share(j):
            share(j, 0, core).wait_send()
            share(j, 1, core).wait_send()

        each(own_pieces, finish_own)
        each(half, finish_relay)
        each(arrivals, finish_share)

    def project_phase(wq_v, w4_v):
        def load_wq(i):
            rows = pl.ds(pl.multiple_of(i * REPACK, REPACK), REPACK)
            return pltpu.make_async_copy(wq_ref.at[rows], w4_v.at[i % 2], wq_sem.at[i % 2])

        load_wq(0).start()
        load_w1.start()
        load_gamma.wait()
        for j in range(half):
            normalise(j)
            to_right(j).start()
            to_left(j).start()
        own_to_partner().start()

        def open_rest(j):
            to_right(half + j).start()
            to_left(half + j).start()

        each(half, open_rest)
        load_wo.start()
        load_w2.start()

        def repack(i):
            @pl.when(i < width // REPACK - 1)
            def _():
                load_wq(i + 1).start()

            load_wq(i).wait()
            rows = pl.ds(pl.multiple_of(i * REPACK, REPACK), REPACK)
            wq_v[rows, :] = w4_v[i % 2].reshape(REPACK, heads * qkv_head)

        each(width // REPACK, repack)
        load_w1.wait()

        def compute_qkv(g):
            slot = g % 2

            @pl.when(g >= own_groups)
            def _():
                for i in range(per_group):
                    lhs_copy(xg_ref.at[rows_at(me, i)], slot, i).wait()

            tile = jnp.dot(lhs[slot], wq_v[...], preferred_element_type=f32).astype(bf16)
            for i in range(per_group):
                qkv_v[group_row(g, i), :] = tile[i * PIECE:(i + 1) * PIECE]

        def step(g):
            ahead = g < groups - LATE

            @pl.when(ahead)
            def _():
                fetch_links(g + 1)

            compute_qkv(g)

            @pl.when(ahead)
            def _():
                fetch_partner(g + 1)

            @pl.when(g < groups - HELD)
            def _():
                compute_up(g)

            @pl.when(jnp.logical_not(ahead) & (g < groups - 1))
            def _():
                fetch_links(g + 1)
                fetch_partner(g + 1)

        each(groups, step)
        for g in range(groups - HELD - 2, groups - HELD):
            wait_out(jnp.int32(g))

    def attend_phase(s_v, o_v, h_v, away, acc, stage, stage_half, x_v, y_v):
        head_dim = qkv_head // 3
        firsts = chunk // FIRST
        blocks = chunk // BLOCK
        cols_half = width // 2
        slices = BLOCK // PIECE
        factor = head_dim ** -0.5 * math.log2(math.e)

        def block_rows(i, size):
            return pl.ds(pl.multiple_of(i * size, size), size)

        def to_partner(p, i, size, side):
            cols = pl.ds(side * cols_half, cols_half)
            src = away.at[pl.ds(0, size), cols]
            dst = rp_ref.at[block_rows(i, size), cols]
            return remote(src, dst, send_p.at[p, side], recv_p.at[p, side], partner)

        def to_side(b, side):
            src = ps_ref.at[block_rows(b, FIRST), pl.ds(side * cols_half, cols_half)]
            dst = ro_ref.at[block_rows(side * firsts + b, FIRST)]
            return remote(src, dst, send_o.at[side, b], recv_o.at[side, b], left if side else right)

        def to_owner(q, k):
            side, block = q % 2, q // 2
            i = block * slices + k
            src = ps_ref.at[block_rows(firsts * FIRST // PIECE + q * slices + k, PIECE)]
            dst = rn_ref.at[block_rows(side * blocks * slices + i, PIECE)]
            device = (chip + 1 + 2 * side) % chips * CORES + core
            return remote(src, dst, send_n.at[side, i], recv_n.at[side, i], device)

        def attend_head(size, rows, head):
            base = pl.multiple_of(head * qkv_head, head_dim)
            q = jnp.concatenate([qkv_v[row, pl.ds(base, head_dim)] for row in rows], axis=0)
            k_cols = pl.ds(pl.multiple_of(base + head_dim, head_dim), head_dim)
            v_cols = pl.ds(pl.multiple_of(base + 2 * head_dim, head_dim), head_dim)
            part = pl.ds(0, 2 * size)
            s = lax.dot_general(q, qkv_v[:, k_cols], (((1,), (1,)), ((), ())), preferred_element_type=f32)
            s_v[part, :] = s
            top = jnp.max(s, axis=-1, keepdims=True)
            e = jnp.exp2((s_v[part, :] - top) * factor)
            total = jnp.sum(e, axis=-1, keepdims=True)
            out = jnp.dot(e.astype(bf16), qkv_v[:, v_cols], preferred_element_type=f32)
            o_v[part, pl.ds(pl.multiple_of(head * head_dim, head_dim), head_dim)] = (out / total).astype(bf16)

        def stage_partner(i, size):
            return pltpu.make_async_copy(rp_ref.at[block_rows(i, size)], stage.at[pl.ds(0, size)], st_sem.at[0])

        def stage_side(side, block):
            src = ro_ref.at[block_rows(side * blocks + block, BLOCK)]
            return pltpu.make_async_copy(src, stage_half, st_sem.at[1])

        def add(size, slot, base, addend):
            def tile(n):
                dst = pl.ds(pl.multiple_of(base + n * LANES, LANES), LANES)
                src = pl.ds(pl.multiple_of(n * LANES, LANES), LANES)
                acc[slot, pl.ds(0, size), dst] += addend[pl.ds(0, size), src]

            each(addend.shape[1] // LANES, tile)

        def spill(slot, i, size):
            return pltpu.make_async_copy(acc.at[slot, pl.ds(0, size)], ps_ref.at[block_rows(i, size)], ps_sem)

        def collect(p, i, size):
            to_partner(p, i, size, 0).wait_recv()
            to_partner(p, i, size, 1).wait_recv()
            stage_partner(i, size).start()

        def sent(p, i, size):
            to_partner(p, i, size, 0).wait_send()
            to_partner(p, i, size, 1).wait_send()

        def partial(size, p, i, chip_offset, block, late, between, flush):
            base = (chip + chip_offset) % chips * CORES
            rows = [block_rows((base + c) * (chunk // size) + block, size) for c in (1 - core, core)]
            loads = [
                pltpu.make_async_copy(h_ref.at[row], h_v.at[pl.ds(n * size, size)], h_sem.at[n])
                for n, row in enumerate(rows)
            ]
            for load in loads:
                load.start()

            def one_head(head):
                pl.when(head == heads - 1)(late)
                attend_head(size, rows, head)

            each(heads, one_head)
            for load in loads:
                load.wait()
            between()
            part = pl.ds(0, 2 * size)
            for n in range(width // COLS):
                cols = pl.ds(n * COLS, COLS)
                both = jnp.dot(
                    o_v[part, :], wo_v[:, cols], preferred_element_type=f32
                ) + jnp.dot(h_v[part, :], w2_v[:, cols], preferred_element_type=f32)
                away[pl.ds(0, size), cols] = both[:size]
                acc[p % 2, pl.ds(0, size), cols] = both[size:]
                to_partner(p, i, size, n).start()
                if n == 0:
                    flush()

        def first_collect(s):
            collect(s, s, FIRST)

        def first_sum(s):
            stage_partner(s, FIRST).wait()
            add(FIRST, s % 2, 0, stage)
            spill(s % 2, s, FIRST).start()

        def first_send(s):
            spill(s % 2, s, FIRST).wait()
            to_side(s, 0).start()
            to_side(s, 1).start()

        def first_step(s):
            @pl.when(s == firsts // 4)
            def _():
                for g in range(groups - HELD, groups):
                    compute_up(jnp.int32(g))

            def late():
                @pl.when(s > 0)
                def _():
                    first_collect(s - 1)

            def between():
                @pl.when(s == 0)
                def _():
                    load_wo.wait()
                    load_w2.wait()

                @pl.when(s == firsts // 4)
                def _():
                    for g in range(groups - HELD, groups):
                        wait_out(jnp.int32(g))

                @pl.when(s > 0)
                def _():
                    sent(s - 1, s - 1, FIRST)
                    first_sum(s - 1)

            def flush():
                @pl.when(s > 0)
                def _():
                    first_send(s - 1)

            partial(FIRST, s, s, 2, s, late, between, flush)

        skip = firsts * FIRST // BLOCK

        def later_parts(q):
            is_mid = q < 2 * blocks
            return is_mid, q % 2, jnp.where(is_mid, q // 2, q - 2 * blocks)

        def later_collect(q):
            is_mid, side, block = later_parts(q)
            collect(firsts + q, skip + q, BLOCK)

            @pl.when(is_mid)
            def _():
                for k in range(BLOCK // FIRST):
                    b = block * (BLOCK // FIRST) + k
                    part = ro_ref.at[block_rows(side * firsts + b, FIRST)]
                    remote(part, part, recv_o.at[side, b], recv_o.at[side, b], partner).wait_recv()
                stage_side(side, block).start()

        def later_sum(q):
            is_mid, side, block = later_parts(q)
            slot = (firsts + q) % 2
            stage_partner(skip + q, BLOCK).wait()
            add(BLOCK, slot, 0, stage)

            @pl.when(is_mid)
            def _():
                stage_side(side, block).wait()
                add(BLOCK, slot, side * cols_half, stage_half)
                spill(slot, skip + q, BLOCK).start()

            @pl.when(jnp.logical_not(is_mid))
            def _():
                def final(k):
                    i = block * slices + k
                    rows = block_rows(i, PIECE)
                    load = pltpu.make_async_copy(x_ref.at[rows], x_v, xr_sem)
                    load.start()
                    copies = []
                    for sd in range(2):
                        src, sem = rn_ref.at[block_rows(sd * blocks * slices + i, PIECE)], recv_n.at[sd, i]
                        remote(src, src, sem, sem, partner).wait_recv()
                        copy = pltpu.make_async_copy(src, stage.at[pl.ds(sd * PIECE, PIECE)], st_sem.at[sd])
                        copy.start()
                        copies.append(copy)
                    load.wait()
                    for copy in copies:
                        copy.wait()

                    def tile(n):
                        cols = pl.ds(pl.multiple_of(n * LANES, LANES), LANES)
                        mine = acc[slot, block_rows(k, PIECE), cols]
                        summed = mine + stage[0:PIECE, cols] + stage[PIECE:2 * PIECE, cols]
                        y_v[:, cols] = (x_v[:, cols].astype(f32) + summed).astype(bf16)

                    each(width // LANES, tile)
                    store = pltpu.make_async_copy(y_v, y_ref.at[rows], y_sem)
                    store.start()
                    store.wait()

                each(slices, final)

        def later_send(q):
            @pl.when(later_parts(q)[0])
            def _():
                spill((firsts + q) % 2, skip + q, BLOCK).wait()
                each(slices, lambda k: to_owner(q, k).start())

        def later_step(q):
            is_mid, side, block = later_parts(q)
            p = firsts + q

            def late():
                @pl.when(q == 0)
                def _():
                    first_collect(jnp.int32(firsts - 1))

                @pl.when(q > 0)
                def _():
                    later_collect(q - 1)

            def between():
                @pl.when(q == 0)
                def _():
                    sent(firsts - 1, firsts - 1, FIRST)
                    first_sum(jnp.int32(firsts - 1))

                @pl.when(q > 0)
                def _():
                    sent(p - 1, skip + q - 1, BLOCK)
                    later_sum(q - 1)

            def flush():
                @pl.when(q == 0)
                def _():
                    first_send(jnp.int32(firsts - 1))

                @pl.when(q > 0)
                def _():
                    later_send(q - 1)

            partial(BLOCK, p, skip + q, jnp.where(is_mid, 1 + 2 * side, 0), block, late, between, flush)

        later = blocks * (chips - 1)
        each(firsts, first_step)
        each(later, later_step)
        later_collect(jnp.int32(later - 1))
        later_sum(jnp.int32(later - 1))
        sent(jnp.int32(firsts + later - 1), jnp.int32(skip + later - 1), BLOCK)

        def finish_side(b):
            to_side(b, 0).wait_send()
            to_side(b, 1).wait_send()

        each(firsts, finish_side)
        each(2 * blocks, lambda q: each(slices, lambda k: to_owner(q, k).wait_send()))

    pl.run_scoped(
        project_phase,
        pltpu.VMEM((width, heads * qkv_head), bf16),
        pltpu.VMEM((2, REPACK, heads, qkv_head), bf16),
    )
    pl.run_scoped(
        attend_phase,
        pltpu.VMEM((2 * BLOCK, qkv_v.shape[0]), f32),
        pltpu.VMEM((2 * BLOCK, wo_v.shape[0]), bf16),
        pltpu.VMEM((2 * BLOCK, h_ref.shape[1]), bf16),
        pltpu.VMEM((BLOCK, width), f32),
        pltpu.VMEM((2, BLOCK, width), f32),
        pltpu.VMEM((BLOCK, width), f32),
        pltpu.VMEM((BLOCK, width // 2), f32),
        pltpu.VMEM((PIECE, width), bf16),
        pltpu.VMEM((PIECE, width), bf16),
    )
    finish_gather()


def transformer_block(chips, x_loc, ln_gamma, w_qkv, w_out, w_up_t, w_down):
    chunk, width = x_loc.shape
    tokens = chunk * chips * CORES
    heads, qkv_head = w_qkv.shape[1], w_qkv.shape[2]
    ff_width = w_up_t.shape[0]
    arrivals = chunk // PIECE + chunk // PIECE // 2
    firsts = chunk // FIRST
    pieces = chunk // PIECE
    pairs = firsts + (chips - 1) * (chunk // BLOCK)
    per_group = GROUP // PIECE
    bf16, f32 = jnp.bfloat16, jnp.float32
    dma = pltpu.SemaphoreType.DMA
    out = pl.pallas_call(
        functools.partial(block_kernel, chips),
        in_specs=[ANY] * 6,
        out_specs=[ANY] * 7,
        out_shape=[
            jax.ShapeDtypeStruct((chunk, width), bf16),
            jax.ShapeDtypeStruct((tokens, width), bf16),
            jax.ShapeDtypeStruct((tokens, ff_width), bf16),
            jax.ShapeDtypeStruct((chips * chunk, width), f32),
            jax.ShapeDtypeStruct((2 * chunk, width // 2), f32),
            jax.ShapeDtypeStruct((2 * chunk, width), f32),
            jax.ShapeDtypeStruct((3 * chunk, width), f32),
        ],
        scratch_shapes=[
            pltpu.VMEM((tokens, heads * qkv_head), bf16),
            pltpu.VMEM(w_out.shape, bf16),
            pltpu.VMEM(w_down.shape, bf16),
            pltpu.VMEM(w_up_t.shape, bf16),
            pltpu.VMEM((2, GROUP, width), bf16),
            pltpu.VMEM((2, GROUP, ff_width), bf16),
            pltpu.VMEM((1, width), f32),
            dma((4,)), dma((pieces,)), dma((2,)), dma((2, per_group)), dma((2, per_group)),
            dma((arrivals,)), dma((arrivals,)), dma((arrivals,)), dma((arrivals,)),
            dma((2 * arrivals + 1,)), dma((2 * arrivals + 1,)),
            dma((2,)), dma((2,)), dma, dma, dma,
            dma((pairs, 2)), dma((pairs, 2)),
            dma((2, firsts)), dma((2, firsts)),
            dma((2, pieces)), dma((2, pieces)),
        ],
        compiler_params=pltpu.CompilerParams(collective_id=0, has_side_effects=True, vmem_limit_bytes=VMEM_LIMIT),
        name="transformer_block",
    )(x_loc, ln_gamma.reshape(1, width), w_qkv, w_out, w_up_t, w_down)
    return out[0]


def solution(mesh):
    chips = mesh.shape["tp"] // CORES

    def local_block(x_loc, ln_gamma, w_qkv, w_out, w_up, w_down):
        heads, head_dim, model_dim = w_out.shape
        return transformer_block(chips, x_loc, ln_gamma, w_qkv, w_out.reshape(heads * head_dim, model_dim), w_up.T, w_down)

    row_spec = P(("data", "tp"), None)
    return jax.shard_map(local_block, mesh=mesh, in_specs=(row_spec, P(None), P(None, "tp", None), P("tp", None, None), P(None, "tp"), P("tp", None)), out_specs=row_spec, check_vma=False)
```

```python
import functools
import math

import jax
import jax.numpy as jnp
from jax import lax
from jax.experimental import pallas as pl
from jax.experimental.pallas import tpu as pltpu
from jax.sharding import PartitionSpec as P

LN_EPS = 1e-6
MESH = pl.DeviceIdType.MESH
CORES = 2
PIECE = 64
GROUP = 256
BLOCK = 128
FIRST = 64
HELD = 2
REPACK = 256
LATE = 4
COLS = 2048
LANES = 512
VMEM_LIMIT = 67_000_000
ANY = pl.BlockSpec(memory_space=pl.ANY)


def neighbours(chips):
    me = lax.axis_index("tp")
    chip, core = me // CORES, me % CORES
    right = (chip + 1) % chips * CORES + core
    left = (chip + chips - 1) % chips * CORES + core
    partner = chip * CORES + (1 - core)
    return me, chip, core, right, left, partner


def greet(devices):
    barrier = pltpu.get_barrier_semaphore()
    for device in devices:
        pl.semaphore_signal(barrier, inc=1, device_id={"tp": device}, device_id_type=MESH)
    pl.semaphore_wait(barrier, len(devices))


def remote(src, dst, send_sem, recv_sem, device):
    return pltpu.make_async_remote_copy(
        src_ref=src, dst_ref=dst, send_sem=send_sem, recv_sem=recv_sem, device_id={"tp": device}, device_id_type=MESH
    )


def each(count, body):
    def step(i, carry):
        body(i)
        return carry

    lax.fori_loop(0, count, step, 0)


def block_kernel(
    chips, x_ref, gamma_ref, wq_ref, wo_ref, w1_ref, w2_ref,
    y_ref, xg_ref, h_ref, rp_ref, ro_ref, rn_ref, ps_ref,
    qkv_v, wo_v, w2_v, w1_v, lhs, ho, gamma_v,
    w_sem, x_sem, wq_sem, lhs_sem, ho_sem, send_r, recv_l, send_l, recv_r, send_g, recv_g,
    h_sem, st_sem, xr_sem, y_sem, ps_sem, send_p, recv_p, send_o, recv_o, send_n, recv_n,
):
    me, chip, core, right, left, partner = neighbours(chips)
    chunk, width = x_ref.shape
    heads, qkv_head = wq_ref.shape[1], wq_ref.shape[2]
    load_wo = pltpu.make_async_copy(wo_ref, wo_v, w_sem.at[1])
    load_w2 = pltpu.make_async_copy(w2_ref, w2_v, w_sem.at[2])
    bf16, f32 = jnp.bfloat16, jnp.float32

    own_pieces = chunk // PIECE
    half = own_pieces // 2
    arrivals = own_pieces + half
    per_group = GROUP // PIECE
    own_groups = chunk // GROUP
    first = own_groups * CORES
    groups = first + arrivals

    def load_x(piece):
        slot, row = piece // per_group, piece % per_group * PIECE
        return pltpu.make_async_copy(x_ref.at[pl.ds(piece * PIECE, PIECE)], lhs.at[slot, pl.ds(row, PIECE)], x_sem.at[piece])

    for j in range(half):
        load_x(j).start()
        load_x(j + half).start()
    load_gamma = pltpu.make_async_copy(gamma_ref, gamma_v, w_sem.at[3])
    load_gamma.start()

    load_w1 = pltpu.make_async_copy(w1_ref, w1_v, w_sem.at[0])
    greet((right, left, partner))

    def rows_at(device, piece):
        return pl.ds(pl.multiple_of(device * chunk + piece * PIECE, PIECE), PIECE)

    def own_send(piece, sends, recvs, j, device):
        rows = xg_ref.at[rows_at(me, piece)]
        return remote(rows, rows, sends.at[j], recvs.at[j], device)

    def opening(side):
        src = lhs.at[side, pl.ds(0, PIECE)]
        dst = xg_ref.at[rows_at(me, side * half)]
        sends, recvs, device = (send_l, recv_r, left) if side else (send_r, recv_l, right)
        return remote(src, dst, sends.at[0], recvs.at[0], device)

    def to_right(j):
        return own_send(j, send_r, recv_l, j, right)

    def to_left(j):
        return own_send((j + half) % own_pieces, send_l, recv_r, j, left)

    def own_to_partner():
        rows = xg_ref.at[pl.ds(pl.multiple_of(me * chunk, chunk), chunk)]
        return remote(rows, rows, send_g.at[2 * arrivals], recv_g.at[2 * arrivals], partner)

    def normalise(j):
        out = []
        for side in range(2):
            rows = pl.ds(j * PIECE, PIECE)
            piece = j + side * half
            load_x(piece).wait()
            vals = lhs[side, rows, :].astype(f32)
            centered = vals - jnp.mean(vals, axis=-1, keepdims=True)
            var = jnp.mean(centered * centered, axis=-1, keepdims=True)
            lhs[side, rows, :] = (centered * lax.rsqrt(var + LN_EPS) * gamma_v[...]).astype(bf16)
            copy = pltpu.make_async_copy(lhs.at[side, rows], xg_ref.at[rows_at(me, piece)], lhs_sem.at[side, 0])
            copy.start()
            out.append(copy)
            if j == 0:
                opening(side).start()
        for copy in out:
            copy.wait()

    def left_row(j, c):
        return ((chip + chips - 1 - j // own_pieces) % chips * CORES + c) * chunk + j % own_pieces * PIECE

    def right_row(j, c):
        return ((chip + 1 + j // own_pieces) % chips * CORES + c) * chunk + (j + half) % own_pieces * PIECE

    def side_rows(j, side, c):
        row = right_row(j, c) if side else left_row(j, c)
        return pl.ds(pl.multiple_of(row, PIECE), PIECE)

    def lhs_copy(src, slot, i):
        return pltpu.make_async_copy(src, lhs.at[slot, pl.ds(i * PIECE, PIECE)], lhs_sem.at[slot, i])

    def relay(j, side):
        rows = xg_ref.at[side_rows(j, side, core)]
        sends, recvs, device = (send_l, recv_r, left) if side else (send_r, recv_l, right)
        return remote(rows, rows, sends.at[own_pieces + j], recvs.at[own_pieces + j], device)

    def share(j, side, c):
        rows = xg_ref.at[side_rows(j, side, c)]
        return remote(rows, rows, send_g.at[2 * j + side], recv_g.at[2 * j + side], partner)

    def fetch_links(g):
        slot = g % 2

        @pl.when((g >= own_groups) & (g < first))
        def _():
            @pl.when(g == own_groups)
            def _():
                for side in range(2):
                    opening(side).wait_send()
                own_to_partner().wait_recv()

            for i in range(per_group):
                lhs_copy(xg_ref.at[rows_at(partner, (g - own_groups) * per_group + i)], slot, i).start()

        @pl.when(g >= first)
        def _():
            j = g - first
            for side in range(2):
                rows = xg_ref.at[side_rows(j, side, core)]
                sem = (recv_r if side else recv_l).at[j]
                remote(rows, rows, sem, sem, partner).wait_recv()

            @pl.when(j < half)
            def _():
                relay(j, 0).start()
                relay(j, 1).start()

            for side in range(2):
                share(j, side, core).start()
                lhs_copy(xg_ref.at[side_rows(j, side, core)], slot, side).start()

    def fetch_partner(g):
        @pl.when(g >= first)
        def _():
            j = g - first
            for side in range(2):
                share(j, side, 1 - core).wait_recv()
            for side in range(2):
                lhs_copy(xg_ref.at[side_rows(j, side, 1 - core)], g % 2, 2 + side).start()

    def group_row(g, i):
        j = g - first
        early = jnp.where(g < own_groups, me, partner) * chunk + ((g % own_groups) * per_group + i) * PIECE
        c = core if i < 2 else 1 - core
        late = right_row(j, c) if i % 2 else left_row(j, c)
        return pl.ds(pl.multiple_of(jnp.where(g < first, early, late), PIECE), PIECE)

    def out_copy(g, i):
        slot = g % 2
        return pltpu.make_async_copy(ho.at[slot, pl.ds(i * PIECE, PIECE)], h_ref.at[group_row(g, i)], ho_sem.at[slot, i])

    def wait_out(g):
        for i in range(per_group):
            out_copy(g, i).wait()

    def compute_up(g):
        slot = g % 2

        @pl.when((g >= 2) & (g < groups - HELD))
        def _():
            wait_out(g - 2)

        pre = lax.dot_general(lhs[slot], w1_v[...], (((1,), (1,)), ((), ())), preferred_element_type=f32)
        ho[slot] = jax.nn.gelu(pre, approximate=True).astype(bf16)
        for i in range(per_group):
            out_copy(g, i).start()

    def finish_gather():
        own_to_partner().wait_send()

        def finish_own(j):
            to_right(j + 1).wait_send()
            to_left(j + 1).wait_send()

        def finish_relay(j):
            relay(j, 0).wait_send()
            relay(j, 1).wait_send()

        def finish_share(j):
            share(j, 0, core).wait_send()
            share(j, 1, core).wait_send()

        each(own_pieces - 1, finish_own)
        each(half, finish_relay)
        each(arrivals, finish_share)

    def project_phase(wq_v, w4_v):
        def load_wq(i):
            rows = pl.ds(pl.multiple_of(i * REPACK, REPACK), REPACK)
            return pltpu.make_async_copy(wq_ref.at[rows], w4_v.at[i % 2], wq_sem.at[i % 2])

        load_wq(0).start()
        load_w1.start()
        load_gamma.wait()
        for j in range(half):
            normalise(j)
            if j > 0:
                to_right(j).start()
                to_left(j).start()
        own_to_partner().start()

        def open_rest(j):
            to_right(half + j).start()
            to_left(half + j).start()

        each(half, open_rest)
        load_wo.start()
        load_w2.start()

        def repack(i):
            @pl.when(i < width // REPACK - 1)
            def _():
                load_wq(i + 1).start()

            load_wq(i).wait()
            rows = pl.ds(pl.multiple_of(i * REPACK, REPACK), REPACK)
            wq_v[rows, :] = w4_v[i % 2].reshape(REPACK, heads * qkv_head)

        each(width // REPACK, repack)
        load_w1.wait()

        def qkv_rows(g, pieces):
            slot = g % 2

            @pl.when(g >= own_groups)
            def _():
                for i in pieces:
                    lhs_copy(xg_ref.at[rows_at(me, i)], slot, i).wait()

            rows = pl.ds(pieces[0] * PIECE, len(pieces) * PIECE)
            tile = jnp.dot(lhs[slot, rows, :], wq_v[...], preferred_element_type=f32).astype(bf16)
            for n, i in enumerate(pieces):
                qkv_v[group_row(g, i), :] = tile[n * PIECE:(n + 1) * PIECE]

        def step(g):
            ahead = g < groups - LATE

            @pl.when(ahead)
            def _():
                fetch_links(g + 1)

            qkv_rows(g, range(per_group))

            @pl.when(jnp.logical_not(ahead))
            def _():
                fetch_links(g + 1)

            @pl.when(ahead)
            def _():
                fetch_partner(g + 1)

            @pl.when(g < groups - HELD)
            def _():
                compute_up(g)

            @pl.when(jnp.logical_not(ahead) & (g < groups - 2))
            def _():
                fetch_partner(g + 1)

        each(groups - 1, step)
        last = jnp.int32(groups - 1)
        qkv_rows(last, range(per_group // 2))
        fetch_partner(last)
        qkv_rows(last, range(per_group // 2, per_group))
        for g in range(groups - HELD - 2, groups - HELD):
            wait_out(jnp.int32(g))

    def attend_phase(s_v, o_v, h_v, away, acc, stage, stage_half, x_v, y_v):
        head_dim = qkv_head // 3
        firsts = chunk // FIRST
        blocks = chunk // BLOCK
        cols_half = width // 2
        slices = BLOCK // PIECE
        factor = head_dim ** -0.5 * math.log2(math.e)

        def block_rows(i, size):
            return pl.ds(pl.multiple_of(i * size, size), size)

        def to_partner(p, i, size, side):
            cols = pl.ds(side * cols_half, cols_half)
            src = away.at[pl.ds(0, size), cols]
            dst = rp_ref.at[block_rows(i, size), cols]
            return remote(src, dst, send_p.at[p, side], recv_p.at[p, side], partner)

        def to_side(b, side):
            src = ps_ref.at[block_rows(b, FIRST), pl.ds(side * cols_half, cols_half)]
            dst = ro_ref.at[block_rows(side * firsts + b, FIRST)]
            return remote(src, dst, send_o.at[side, b], recv_o.at[side, b], left if side else right)

        def to_owner(q, k):
            side, block = q % 2, q // 2
            i = block * slices + k
            src = ps_ref.at[block_rows(firsts * FIRST // PIECE + q * slices + k, PIECE)]
            dst = rn_ref.at[block_rows(side * blocks * slices + i, PIECE)]
            device = (chip + 1 + 2 * side) % chips * CORES + core
            return remote(src, dst, send_n.at[side, i], recv_n.at[side, i], device)

        def attend_head(size, rows, head):
            base = pl.multiple_of(head * qkv_head, head_dim)
            q = jnp.concatenate([qkv_v[row, pl.ds(base, head_dim)] for row in rows], axis=0)
            k_cols = pl.ds(pl.multiple_of(base + head_dim, head_dim), head_dim)
            v_cols = pl.ds(pl.multiple_of(base + 2 * head_dim, head_dim), head_dim)
            part = pl.ds(0, 2 * size)
            s = lax.dot_general(q, qkv_v[:, k_cols], (((1,), (1,)), ((), ())), preferred_element_type=f32)
            s_v[part, :] = s
            top = jnp.max(s, axis=-1, keepdims=True)
            e = jnp.exp2((s_v[part, :] - top) * factor)
            total = jnp.sum(e, axis=-1, keepdims=True)
            out = jnp.dot(e.astype(bf16), qkv_v[:, v_cols], preferred_element_type=f32)
            o_v[part, pl.ds(pl.multiple_of(head * head_dim, head_dim), head_dim)] = (out / total).astype(bf16)

        def stage_partner(i, size):
            return pltpu.make_async_copy(rp_ref.at[block_rows(i, size)], stage.at[pl.ds(0, size)], st_sem.at[0])

        def stage_side(side, block):
            src = ro_ref.at[block_rows(side * blocks + block, BLOCK)]
            return pltpu.make_async_copy(src, stage_half, st_sem.at[1])

        def add(size, slot, base, addend):
            def tile(n):
                dst = pl.ds(pl.multiple_of(base + n * LANES, LANES), LANES)
                src = pl.ds(pl.multiple_of(n * LANES, LANES), LANES)
                acc[slot, pl.ds(0, size), dst] += addend[pl.ds(0, size), src]

            each(addend.shape[1] // LANES, tile)

        def spill(slot, i, size):
            return pltpu.make_async_copy(acc.at[slot, pl.ds(0, size)], ps_ref.at[block_rows(i, size)], ps_sem)

        def collect(p, i, size):
            to_partner(p, i, size, 0).wait_recv()
            to_partner(p, i, size, 1).wait_recv()
            stage_partner(i, size).start()

        def sent(p, i, size):
            to_partner(p, i, size, 0).wait_send()
            to_partner(p, i, size, 1).wait_send()

        def partial(size, p, i, chip_offset, block, gather, total, between):
            base = (chip + chip_offset) % chips * CORES
            rows = [block_rows((base + c) * (chunk // size) + block, size) for c in (1 - core, core)]
            loads = [
                pltpu.make_async_copy(h_ref.at[row], h_v.at[pl.ds(n * size, size)], h_sem.at[n])
                for n, row in enumerate(rows)
            ]
            def one_head(head):
                @pl.when(head == heads - 2)
                def _():
                    gather()
                    for load in loads:
                        load.start()

                pl.when(head == heads - 1)(total)
                attend_head(size, rows, head)

            each(heads, one_head)
            for load in loads:
                load.wait()
            between()
            part = pl.ds(0, 2 * size)
            for n in range(width // COLS):
                cols = pl.ds(n * COLS, COLS)
                both = jnp.dot(
                    o_v[part, :], wo_v[:, cols], preferred_element_type=f32
                ) + jnp.dot(h_v[part, :], w2_v[:, cols], preferred_element_type=f32)
                away[pl.ds(0, size), cols] = both[:size]
                acc[p % 2, pl.ds(0, size), cols] = both[size:]
                to_partner(p, i, size, n).start()

        def first_collect(s):
            collect(s, s, FIRST)

        def first_sum(s):
            stage_partner(s, FIRST).wait()
            add(FIRST, s % 2, 0, stage)
            spill(s % 2, s, FIRST).start()

        def first_send(s):
            spill(s % 2, s, FIRST).wait()
            to_side(s, 0).start()
            to_side(s, 1).start()

        def first_step(s):
            held = s - firsts // 4
            has_held = (held >= 0) & (held < HELD)

            @pl.when(has_held)
            def _():
                compute_up(groups - HELD + held)

            def gather():
                @pl.when(has_held)
                def _():
                    wait_out(groups - HELD + held)

                @pl.when(s > 0)
                def _():
                    first_collect(s - 1)

            def total():
                @pl.when(s > 0)
                def _():
                    first_sum(s - 1)

            def between():
                @pl.when(s == 0)
                def _():
                    load_wo.wait()
                    load_w2.wait()

                @pl.when(s > 0)
                def _():
                    sent(s - 1, s - 1, FIRST)
                    first_send(s - 1)

            partial(FIRST, s, s, 2, s, gather, total, between)

        skip = firsts * FIRST // BLOCK

        def later_parts(q):
            is_mid = q < 2 * blocks
            return is_mid, q % 2, jnp.where(is_mid, q // 2, q - 2 * blocks)

        def later_collect(q):
            is_mid, side, block = later_parts(q)
            collect(firsts + q, skip + q, BLOCK)

            @pl.when(is_mid)
            def _():
                for k in range(BLOCK // FIRST):
                    b = block * (BLOCK // FIRST) + k
                    part = ro_ref.at[block_rows(side * firsts + b, FIRST)]
                    remote(part, part, recv_o.at[side, b], recv_o.at[side, b], partner).wait_recv()
                stage_side(side, block).start()

        def later_sum(q):
            is_mid, side, block = later_parts(q)
            slot = (firsts + q) % 2
            stage_partner(skip + q, BLOCK).wait()
            add(BLOCK, slot, 0, stage)

            @pl.when(is_mid)
            def _():
                stage_side(side, block).wait()
                add(BLOCK, slot, side * cols_half, stage_half)
                spill(slot, skip + q, BLOCK).start()

            @pl.when(jnp.logical_not(is_mid))
            def _():
                def final(k):
                    i = block * slices + k
                    rows = block_rows(i, PIECE)
                    load = pltpu.make_async_copy(x_ref.at[rows], x_v, xr_sem)
                    load.start()
                    copies = []
                    for sd in range(2):
                        src, sem = rn_ref.at[block_rows(sd * blocks * slices + i, PIECE)], recv_n.at[sd, i]
                        remote(src, src, sem, sem, partner).wait_recv()
                        copy = pltpu.make_async_copy(src, stage.at[pl.ds(sd * PIECE, PIECE)], st_sem.at[sd])
                        copy.start()
                        copies.append(copy)
                    load.wait()
                    for copy in copies:
                        copy.wait()

                    def tile(n):
                        cols = pl.ds(pl.multiple_of(n * LANES, LANES), LANES)
                        mine = acc[slot, block_rows(k, PIECE), cols]
                        summed = mine + stage[0:PIECE, cols] + stage[PIECE:2 * PIECE, cols]
                        y_v[:, cols] = (x_v[:, cols].astype(f32) + summed).astype(bf16)

                    each(width // LANES, tile)
                    store = pltpu.make_async_copy(y_v, y_ref.at[rows], y_sem)
                    store.start()
                    store.wait()

                each(slices, final)

        def later_send(q):
            @pl.when(later_parts(q)[0])
            def _():
                spill((firsts + q) % 2, skip + q, BLOCK).wait()
                each(slices, lambda k: to_owner(q, k).start())

        def later_step(q):
            is_mid, side, block = later_parts(q)
            p = firsts + q

            def gather():
                @pl.when(q == 0)
                def _():
                    first_collect(jnp.int32(firsts - 1))

                @pl.when(q > 0)
                def _():
                    later_collect(q - 1)

            def total():
                @pl.when(q == 0)
                def _():
                    first_sum(jnp.int32(firsts - 1))

                @pl.when(q > 0)
                def _():
                    later_sum(q - 1)

            def between():
                @pl.when(q == 0)
                def _():
                    sent(firsts - 1, firsts - 1, FIRST)
                    first_send(jnp.int32(firsts - 1))

                @pl.when(q > 0)
                def _():
                    sent(p - 1, skip + q - 1, BLOCK)
                    later_send(q - 1)

            partial(BLOCK, p, skip + q, jnp.where(is_mid, 1 + 2 * side, 0), block, gather, total, between)

        later = blocks * (chips - 1)
        each(firsts, first_step)
        each(later, later_step)
        later_collect(jnp.int32(later - 1))
        later_sum(jnp.int32(later - 1))
        sent(jnp.int32(firsts + later - 1), jnp.int32(skip + later - 1), BLOCK)

        def finish_side(b):
            to_side(b, 0).wait_send()
            to_side(b, 1).wait_send()

        each(firsts, finish_side)
        each(2 * blocks, lambda q: each(slices, lambda k: to_owner(q, k).wait_send()))

    pl.run_scoped(
        project_phase,
        pltpu.VMEM((width, heads * qkv_head), bf16),
        pltpu.VMEM((2, REPACK, heads, qkv_head), bf16),
    )
    pl.run_scoped(
        attend_phase,
        pltpu.VMEM((2 * BLOCK, qkv_v.shape[0]), f32),
        pltpu.VMEM((2 * BLOCK, wo_v.shape[0]), bf16),
        pltpu.VMEM((2 * BLOCK, h_ref.shape[1]), bf16),
        pltpu.VMEM((BLOCK, width), f32),
        pltpu.VMEM((2, BLOCK, width), f32),
        pltpu.VMEM((BLOCK, width), f32),
        pltpu.VMEM((BLOCK, width // 2), f32),
        pltpu.VMEM((PIECE, width), bf16),
        pltpu.VMEM((PIECE, width), bf16),
    )
    finish_gather()


def transformer_block(chips, x_loc, ln_gamma, w_qkv, w_out, w_up_t, w_down):
    chunk, width = x_loc.shape
    tokens = chunk * chips * CORES
    heads, qkv_head = w_qkv.shape[1], w_qkv.shape[2]
    ff_width = w_up_t.shape[0]
    arrivals = chunk // PIECE + chunk // PIECE // 2
    firsts = chunk // FIRST
    pieces = chunk // PIECE
    pairs = firsts + (chips - 1) * (chunk // BLOCK)
    per_group = GROUP // PIECE
    bf16, f32 = jnp.bfloat16, jnp.float32
    dma = pltpu.SemaphoreType.DMA
    out = pl.pallas_call(
        functools.partial(block_kernel, chips),
        in_specs=[ANY] * 6,
        out_specs=[ANY] * 7,
        out_shape=[
            jax.ShapeDtypeStruct((chunk, width), bf16),
            jax.ShapeDtypeStruct((tokens, width), bf16),
            jax.ShapeDtypeStruct((tokens, ff_width), bf16),
            jax.ShapeDtypeStruct((chips * chunk, width), f32),
            jax.ShapeDtypeStruct((2 * chunk, width // 2), f32),
            jax.ShapeDtypeStruct((2 * chunk, width), f32),
            jax.ShapeDtypeStruct((3 * chunk, width), f32),
        ],
        scratch_shapes=[
            pltpu.VMEM((tokens, heads * qkv_head), bf16),
            pltpu.VMEM(w_out.shape, bf16),
            pltpu.VMEM(w_down.shape, bf16),
            pltpu.VMEM(w_up_t.shape, bf16),
            pltpu.VMEM((2, GROUP, width), bf16),
            pltpu.VMEM((2, GROUP, ff_width), bf16),
            pltpu.VMEM((1, width), f32),
            dma((4,)), dma((pieces,)), dma((2,)), dma((2, per_group)), dma((2, per_group)),
            dma((arrivals,)), dma((arrivals,)), dma((arrivals,)), dma((arrivals,)),
            dma((2 * arrivals + 1,)), dma((2 * arrivals + 1,)),
            dma((2,)), dma((2,)), dma, dma, dma,
            dma((pairs, 2)), dma((pairs, 2)),
            dma((2, firsts)), dma((2, firsts)),
            dma((2, pieces)), dma((2, pieces)),
        ],
        compiler_params=pltpu.CompilerParams(collective_id=0, has_side_effects=True, vmem_limit_bytes=VMEM_LIMIT),
        name="transformer_block",
    )(x_loc, ln_gamma.reshape(1, width), w_qkv, w_out, w_up_t, w_down)
    return out[0]


def solution(mesh):
    chips = mesh.shape["tp"] // CORES

    def local_block(x_loc, ln_gamma, w_qkv, w_out, w_up, w_down):
        heads, head_dim, model_dim = w_out.shape
        return transformer_block(chips, x_loc, ln_gamma, w_qkv, w_out.reshape(heads * head_dim, model_dim), w_up.T, w_down)

    row_spec = P(("data", "tp"), None)
    return jax.shard_map(local_block, mesh=mesh, in_specs=(row_spec, P(None), P(None, "tp", None), P("tp", None, None), P(None, "tp"), P("tp", None)), out_specs=row_spec, check_vma=False)
```

```python
import functools
import math

import jax
import jax.numpy as jnp
from jax import lax
from jax.experimental import pallas as pl
from jax.experimental.pallas import tpu as pltpu
from jax.sharding import PartitionSpec as P

LN_EPS = 1e-6
MESH = pl.DeviceIdType.MESH
CORES = 2
PIECE = 64
GROUP = 256
BLOCK = 128
FIRST = 64
HELD = 2
REPACK = 256
DIRECT = 4
LATE = 4
COLS = 2048
LANES = 512
VMEM_LIMIT = 67_000_000
ANY = pl.BlockSpec(memory_space=pl.ANY)


def neighbours(chips):
    me = lax.axis_index("tp")
    chip, core = me // CORES, me % CORES
    right = (chip + 1) % chips * CORES + core
    left = (chip + chips - 1) % chips * CORES + core
    partner = chip * CORES + (1 - core)
    return me, chip, core, right, left, partner


def greet(devices):
    barrier = pltpu.get_barrier_semaphore()
    for device in devices:
        pl.semaphore_signal(barrier, inc=1, device_id={"tp": device}, device_id_type=MESH)
    pl.semaphore_wait(barrier, len(devices))


def remote(src, dst, send_sem, recv_sem, device):
    return pltpu.make_async_remote_copy(
        src_ref=src, dst_ref=dst, send_sem=send_sem, recv_sem=recv_sem, device_id={"tp": device}, device_id_type=MESH
    )


def each(count, body):
    def step(i, carry):
        body(i)
        return carry

    lax.fori_loop(0, count, step, 0)


def block_kernel(
    chips, x_ref, gamma_ref, wq_ref, wo_ref, w1_ref, w2_ref,
    y_ref, xg_ref, h_ref, rp_ref, ro_ref, rn_ref, ps_ref,
    qkv_v, wo_v, w2_v, w1_v, lhs, ho, gamma_v,
    w_sem, x_sem, wq_sem, lhs_sem, ho_sem, send_r, recv_l, send_l, recv_r, send_g, recv_g,
    h_sem, st_sem, xr_sem, y_sem, ps_sem, send_p, recv_p, send_o, recv_o, send_n, recv_n,
):
    me, chip, core, right, left, partner = neighbours(chips)
    chunk, width = x_ref.shape
    heads, qkv_head = wq_ref.shape[1], wq_ref.shape[2]
    load_wo = pltpu.make_async_copy(wo_ref, wo_v, w_sem.at[1])
    load_w2 = pltpu.make_async_copy(w2_ref, w2_v, w_sem.at[2])
    bf16, f32 = jnp.bfloat16, jnp.float32

    own_pieces = chunk // PIECE
    half = own_pieces // 2
    arrivals = own_pieces + half
    per_group = GROUP // PIECE
    own_groups = chunk // GROUP
    first = own_groups * CORES
    groups = first + arrivals

    def load_x(piece):
        slot, row = piece // per_group, piece % per_group * PIECE
        return pltpu.make_async_copy(x_ref.at[pl.ds(piece * PIECE, PIECE)], lhs.at[slot, pl.ds(row, PIECE)], x_sem.at[piece])

    for j in range(half):
        load_x(j).start()
        load_x(j + half).start()
    load_gamma = pltpu.make_async_copy(gamma_ref, gamma_v, w_sem.at[3])
    load_gamma.start()

    load_w1 = pltpu.make_async_copy(w1_ref, w1_v, w_sem.at[0])
    greet((right, left, partner))

    def rows_at(device, piece):
        return pl.ds(pl.multiple_of(device * chunk + piece * PIECE, PIECE), PIECE)

    def own_send(piece, sends, recvs, j, device):
        rows = xg_ref.at[rows_at(me, piece)]
        return remote(rows, rows, sends.at[j], recvs.at[j], device)

    def opening(side):
        src = lhs.at[side, pl.ds(0, PIECE)]
        dst = xg_ref.at[rows_at(me, side * half)]
        sends, recvs, device = (send_l, recv_r, left) if side else (send_r, recv_l, right)
        return remote(src, dst, sends.at[0], recvs.at[0], device)

    def to_right(j):
        return own_send(j, send_r, recv_l, j, right)

    def to_left(j):
        return own_send((j + half) % own_pieces, send_l, recv_r, j, left)

    def own_to_partner():
        rows = xg_ref.at[pl.ds(pl.multiple_of(me * chunk, chunk), chunk)]
        return remote(rows, rows, send_g.at[2 * arrivals], recv_g.at[2 * arrivals], partner)

    def normalise(j):
        out = []
        for side in range(2):
            rows = pl.ds(j * PIECE, PIECE)
            piece = j + side * half
            load_x(piece).wait()
            vals = lhs[side, rows, :].astype(f32)
            centered = vals - jnp.mean(vals, axis=-1, keepdims=True)
            var = jnp.mean(centered * centered, axis=-1, keepdims=True)
            lhs[side, rows, :] = (centered * lax.rsqrt(var + LN_EPS) * gamma_v[...]).astype(bf16)
            copy = pltpu.make_async_copy(lhs.at[side, rows], xg_ref.at[rows_at(me, piece)], lhs_sem.at[side, 0])
            copy.start()
            out.append(copy)
            if j == 0:
                opening(side).start()
        for copy in out:
            copy.wait()

    def left_row(j, c):
        return ((chip + chips - 1 - j // own_pieces) % chips * CORES + c) * chunk + j % own_pieces * PIECE

    def right_row(j, c):
        return ((chip + 1 + j // own_pieces) % chips * CORES + c) * chunk + (j + half) % own_pieces * PIECE

    def side_rows(j, side, c):
        row = right_row(j, c) if side else left_row(j, c)
        return pl.ds(pl.multiple_of(row, PIECE), PIECE)

    def lhs_copy(src, slot, i):
        return pltpu.make_async_copy(src, lhs.at[slot, pl.ds(i * PIECE, PIECE)], lhs_sem.at[slot, i])

    def relay(j, side):
        rows = xg_ref.at[side_rows(j, side, core)]
        sends, recvs, device = (send_l, recv_r, left) if side else (send_r, recv_l, right)
        return remote(rows, rows, sends.at[own_pieces + j], recvs.at[own_pieces + j], device)

    def share(j, side, c):
        rows = xg_ref.at[side_rows(j, side, c)]
        return remote(rows, rows, send_g.at[2 * j + side], recv_g.at[2 * j + side], partner)

    def fetch_links(g):
        slot = g % 2

        @pl.when((g >= own_groups) & (g < first))
        def _():
            @pl.when(g == own_groups)
            def _():
                for side in range(2):
                    opening(side).wait_send()
                own_to_partner().wait_recv()

            for i in range(per_group):
                lhs_copy(xg_ref.at[rows_at(partner, (g - own_groups) * per_group + i)], slot, i).start()

        @pl.when(g >= first)
        def _():
            j = g - first
            for side in range(2):
                rows = xg_ref.at[side_rows(j, side, core)]
                sem = (recv_r if side else recv_l).at[j]
                remote(rows, rows, sem, sem, partner).wait_recv()

            @pl.when(j < half)
            def _():
                relay(j, 0).start()
                relay(j, 1).start()

            for side in range(2):
                share(j, side, core).start()
                lhs_copy(xg_ref.at[side_rows(j, side, core)], slot, side).start()

    def fetch_partner(g):
        @pl.when(g >= first)
        def _():
            j = g - first
            for side in range(2):
                share(j, side, 1 - core).wait_recv()
            for side in range(2):
                lhs_copy(xg_ref.at[side_rows(j, side, 1 - core)], g % 2, 2 + side).start()

    def group_row(g, i):
        j = g - first
        early = jnp.where(g < own_groups, me, partner) * chunk + ((g % own_groups) * per_group + i) * PIECE
        c = core if i < 2 else 1 - core
        late = right_row(j, c) if i % 2 else left_row(j, c)
        return pl.ds(pl.multiple_of(jnp.where(g < first, early, late), PIECE), PIECE)

    def out_copy(g, i):
        slot = g % 2
        return pltpu.make_async_copy(ho.at[slot, pl.ds(i * PIECE, PIECE)], h_ref.at[group_row(g, i)], ho_sem.at[slot, i])

    def wait_out(g):
        for i in range(per_group):
            out_copy(g, i).wait()

    def compute_up(g):
        slot = g % 2

        @pl.when((g >= 2) & (g < groups - HELD))
        def _():
            wait_out(g - 2)

        pre = lax.dot_general(lhs[slot], w1_v[...], (((1,), (1,)), ((), ())), preferred_element_type=f32)
        ho[slot] = jax.nn.gelu(pre, approximate=True).astype(bf16)
        for i in range(per_group):
            out_copy(g, i).start()

    def finish_gather():
        own_to_partner().wait_send()

        def finish_own(j):
            to_right(j + 1).wait_send()
            to_left(j + 1).wait_send()

        def finish_relay(j):
            relay(j, 0).wait_send()
            relay(j, 1).wait_send()

        def finish_share(j):
            share(j, 0, core).wait_send()
            share(j, 1, core).wait_send()

        each(own_pieces - 1, finish_own)
        each(half, finish_relay)
        each(arrivals, finish_share)

    def project_phase(wq_v, w4_v):
        def load_wq(i):
            rows = pl.ds(pl.multiple_of(i * REPACK, REPACK), REPACK)
            return pltpu.make_async_copy(wq_ref.at[rows], w4_v.at[i % 2], wq_sem.at[i % 2])

        load_wq(0).start()
        load_w1.start()
        load_gamma.wait()
        for j in range(half):
            normalise(j)
            if j > 0:
                to_right(j).start()
                to_left(j).start()
        own_to_partner().start()

        def open_rest(j):
            to_right(half + j).start()
            to_left(half + j).start()

        each(half, open_rest)
        load_wo.start()
        load_w2.start()

        def repack(i):
            @pl.when(i < width // REPACK - 1)
            def _():
                load_wq(i + 1).start()

            load_wq(i).wait()
            rows = pl.ds(pl.multiple_of(i * REPACK, REPACK), REPACK)
            wq_v[rows, :] = w4_v[i % 2].reshape(REPACK, heads * qkv_head)

        each(width // REPACK, repack)
        load_w1.wait()

        def qkv_rows(g, pieces):
            slot = g % 2

            @pl.when(g >= own_groups)
            def _():
                for i in pieces:
                    lhs_copy(xg_ref.at[rows_at(me, i)], slot, i).wait()

            rows = pl.ds(pieces[0] * PIECE, len(pieces) * PIECE)
            tile = jnp.dot(lhs[slot, rows, :], wq_v[...], preferred_element_type=f32).astype(bf16)
            for n, i in enumerate(pieces):
                qkv_v[group_row(g, i), :] = tile[n * PIECE:(n + 1) * PIECE]

        def step(g):
            ahead = g < groups - LATE

            @pl.when(ahead)
            def _():
                fetch_links(g + 1)

            qkv_rows(g, range(per_group))

            @pl.when(jnp.logical_not(ahead))
            def _():
                fetch_links(g + 1)

            @pl.when(ahead)
            def _():
                fetch_partner(g + 1)

            @pl.when(g < groups - HELD)
            def _():
                compute_up(g)

            @pl.when(jnp.logical_not(ahead) & (g < groups - 2))
            def _():
                fetch_partner(g + 1)

        each(groups - 1, step)
        last = jnp.int32(groups - 1)
        qkv_rows(last, range(per_group // 2))
        fetch_partner(last)
        qkv_rows(last, range(per_group // 2, per_group))
        for g in range(groups - HELD - 2, groups - HELD):
            wait_out(jnp.int32(g))

    def attend_phase(s_v, o_v, h_v, away, acc, stage, stage_half, x_v, y_v):
        head_dim = qkv_head // 3
        firsts = chunk // FIRST
        blocks = chunk // BLOCK
        cols_half = width // 2
        slices = BLOCK // PIECE
        factor = head_dim ** -0.5 * math.log2(math.e)

        def block_rows(i, size):
            return pl.ds(pl.multiple_of(i * size, size), size)

        def to_partner(p, i, size, side):
            cols = pl.ds(side * cols_half, cols_half)
            src = away.at[pl.ds(0, size), cols]
            dst = rp_ref.at[block_rows(i, size), cols]
            return remote(src, dst, send_p.at[p, side], recv_p.at[p, side], partner)

        def to_side(b, side):
            src = ps_ref.at[block_rows(b, FIRST), pl.ds(side * cols_half, cols_half)]
            dst = ro_ref.at[block_rows(side * firsts + b, FIRST)]
            return remote(src, dst, send_o.at[side, b], recv_o.at[side, b], left if side else right)

        def to_owner(q, k):
            side, block = (q + core) % 2, q // 2
            i = block * slices + k
            src = ps_ref.at[block_rows(firsts * FIRST // PIECE + q * slices + k, PIECE)]
            dst = rn_ref.at[block_rows(side * blocks * slices + i, PIECE)]
            device = (chip + 1 + 2 * side) % chips * CORES + core
            return remote(src, dst, send_n.at[side, i], recv_n.at[side, i], device)

        def attend_head(size, rows, head):
            base = pl.multiple_of(head * qkv_head, head_dim)
            q = jnp.concatenate([qkv_v[row, pl.ds(base, head_dim)] for row in rows], axis=0)
            k_cols = pl.ds(pl.multiple_of(base + head_dim, head_dim), head_dim)
            v_cols = pl.ds(pl.multiple_of(base + 2 * head_dim, head_dim), head_dim)
            part = pl.ds(0, 2 * size)
            s = lax.dot_general(q, qkv_v[:, k_cols], (((1,), (1,)), ((), ())), preferred_element_type=f32)
            s_v[part, :] = s
            top = jnp.max(s, axis=-1, keepdims=True)
            e = jnp.exp2((s_v[part, :] - top) * factor)
            total = jnp.sum(e, axis=-1, keepdims=True)
            out = jnp.dot(e.astype(bf16), qkv_v[:, v_cols], preferred_element_type=f32)
            o_v[part, pl.ds(pl.multiple_of(head * head_dim, head_dim), head_dim)] = (out / total).astype(bf16)

        def stage_partner(i, size):
            return pltpu.make_async_copy(rp_ref.at[block_rows(i, size)], stage.at[pl.ds(0, size)], st_sem.at[0])

        def stage_side(side, block):
            src = ro_ref.at[block_rows(side * blocks + block, BLOCK)]
            return pltpu.make_async_copy(src, stage_half, st_sem.at[1])

        def add(size, slot, base, addend):
            def tile(n):
                dst = pl.ds(pl.multiple_of(base + n * LANES, LANES), LANES)
                src = pl.ds(pl.multiple_of(n * LANES, LANES), LANES)
                acc[slot, pl.ds(0, size), dst] += addend[pl.ds(0, size), src]

            each(addend.shape[1] // LANES, tile)

        def spill(slot, i, size):
            return pltpu.make_async_copy(acc.at[slot, pl.ds(0, size)], ps_ref.at[block_rows(i, size)], ps_sem)

        def collect(p, i, size):
            to_partner(p, i, size, 0).wait_recv()
            to_partner(p, i, size, 1).wait_recv()
            stage_partner(i, size).start()

        def sent(p, i, size):
            to_partner(p, i, size, 0).wait_send()
            to_partner(p, i, size, 1).wait_send()

        def partial(size, p, i, offsets, block, gather, total, between):
            devices = [(chip + offset) % chips * CORES + c for offset, c in zip(offsets, (1 - core, core))]
            rows = [block_rows(device * (chunk // size) + block, size) for device in devices]
            loads = [
                pltpu.make_async_copy(h_ref.at[row], h_v.at[pl.ds(n * size, size)], h_sem.at[n])
                for n, row in enumerate(rows)
            ]
            def one_head(head):
                @pl.when(head == heads - 2)
                def _():
                    gather()
                    for load in loads:
                        load.start()

                pl.when(head == heads - 1)(total)
                attend_head(size, rows, head)

            each(heads, one_head)
            for load in loads:
                load.wait()
            between()
            part = pl.ds(0, 2 * size)
            for n in range(width // COLS):
                cols = pl.ds(n * COLS, COLS)
                both = jnp.dot(
                    o_v[part, :], wo_v[:, cols], preferred_element_type=f32
                ) + jnp.dot(h_v[part, :], w2_v[:, cols], preferred_element_type=f32)
                away[pl.ds(0, size), cols] = both[:size]
                acc[p % 2, pl.ds(0, size), cols] = both[size:]
                to_partner(p, i, size, n).start()

        def first_collect(s):
            collect(s, s, FIRST)

        def opening_sum(s, side):
            src = acc.at[s % 2, pl.ds(0, FIRST), pl.ds(side * cols_half, cols_half)]
            dst = ro_ref.at[block_rows(side * firsts + s, FIRST)]
            return remote(src, dst, send_o.at[side, s], recv_o.at[side, s], left if side else right)

        def first_sum(s):
            stage_partner(s, FIRST).wait()
            add(FIRST, s % 2, 0, stage)

            @pl.when(s < DIRECT)
            def _():
                opening_sum(s, 0).start()
                opening_sum(s, 1).start()

            @pl.when(s >= DIRECT)
            def _():
                spill(s % 2, s, FIRST).start()

        def first_send(s):
            @pl.when(s >= DIRECT)
            def _():
                spill(s % 2, s, FIRST).wait()
                to_side(s, 0).start()
                to_side(s, 1).start()

        def first_step(s):
            held = s - firsts // 4
            has_held = (held >= 0) & (held < HELD)

            @pl.when(has_held)
            def _():
                compute_up(groups - HELD + held)

            def gather():
                @pl.when(has_held)
                def _():
                    wait_out(groups - HELD + held)

                @pl.when(s > 0)
                def _():
                    first_collect(s - 1)

            def total():
                @pl.when(s > 0)
                def _():
                    first_sum(s - 1)

            def between():
                @pl.when(s == 0)
                def _():
                    load_wo.wait()
                    load_w2.wait()

                @pl.when(s > 0)
                def _():
                    sent(s - 1, s - 1, FIRST)
                    first_send(s - 1)

                @pl.when((s >= 2) & (s < DIRECT + 2))
                def _():
                    opening_sum(s - 2, 0).wait_send()
                    opening_sum(s - 2, 1).wait_send()

            partial(FIRST, s, s, (2, 2), s, gather, total, between)

        skip = firsts * FIRST // BLOCK

        def later_parts(q):
            is_mid = q < 2 * blocks
            return is_mid, (q + core) % 2, jnp.where(is_mid, q // 2, q - 2 * blocks)

        def later_collect(q):
            is_mid, side, block = later_parts(q)
            collect(firsts + q, skip + q, BLOCK)

            @pl.when(is_mid)
            def _():
                for k in range(BLOCK // FIRST):
                    b = block * (BLOCK // FIRST) + k
                    part = ro_ref.at[block_rows(side * firsts + b, FIRST)]
                    remote(part, part, recv_o.at[side, b], recv_o.at[side, b], partner).wait_recv()
                stage_side(side, block).start()

        def later_sum(q):
            is_mid, side, block = later_parts(q)
            slot = (firsts + q) % 2
            stage_partner(skip + q, BLOCK).wait()
            add(BLOCK, slot, 0, stage)

            @pl.when(is_mid)
            def _():
                stage_side(side, block).wait()
                add(BLOCK, slot, side * cols_half, stage_half)

            spill(slot, skip + q, BLOCK).start()

        def final(i):
            rows = block_rows(i, PIECE)
            load = pltpu.make_async_copy(x_ref.at[rows], x_v, xr_sem)
            load.start()
            first_own = (skip + 2 * blocks) * slices
            own = pltpu.make_async_copy(ps_ref.at[block_rows(first_own + i, PIECE)], acc.at[0, pl.ds(0, PIECE)], ps_sem)
            own.start()
            copies = []
            for sd in range(2):
                src, sem = rn_ref.at[block_rows(sd * blocks * slices + i, PIECE)], recv_n.at[sd, i]
                remote(src, src, sem, sem, partner).wait_recv()
                copy = pltpu.make_async_copy(src, stage.at[pl.ds(sd * PIECE, PIECE)], st_sem.at[sd])
                copy.start()
                copies.append(copy)
            load.wait()
            own.wait()
            for copy in copies:
                copy.wait()

            def tile(n):
                cols = pl.ds(pl.multiple_of(n * LANES, LANES), LANES)
                summed = acc[0, 0:PIECE, cols] + stage[0:PIECE, cols] + stage[PIECE:2 * PIECE, cols]
                y_v[:, cols] = (x_v[:, cols].astype(f32) + summed).astype(bf16)

            each(width // LANES, tile)
            store = pltpu.make_async_copy(y_v, y_ref.at[rows], y_sem)
            store.start()
            store.wait()

        def later_send(q):
            spill((firsts + q) % 2, skip + q, BLOCK).wait()

            @pl.when(later_parts(q)[0])
            def _():
                each(slices, lambda k: to_owner(q, k).start())

        def later_step(q):
            is_mid, side, block = later_parts(q)
            p = firsts + q

            def gather():
                @pl.when(q == 0)
                def _():
                    first_collect(jnp.int32(firsts - 1))

                @pl.when(q > 0)
                def _():
                    later_collect(q - 1)

            def total():
                @pl.when(q == 0)
                def _():
                    first_sum(jnp.int32(firsts - 1))

                @pl.when(q > 0)
                def _():
                    later_sum(q - 1)

            def between():
                @pl.when(q == 0)
                def _():
                    sent(firsts - 1, firsts - 1, FIRST)
                    first_send(jnp.int32(firsts - 1))

                @pl.when(q > 0)
                def _():
                    sent(p - 1, skip + q - 1, BLOCK)
                    later_send(q - 1)

            offsets = [jnp.where(is_mid, 1 + 2 * sd, 0) for sd in (1 - side, side)]
            partial(BLOCK, p, skip + q, offsets, block, gather, total, between)

        later = blocks * (chips - 1)
        each(firsts, first_step)
        each(later, later_step)

        def finish_side(b):
            to_side(b + DIRECT, 0).wait_send()
            to_side(b + DIRECT, 1).wait_send()

        finish_gather()
        each(firsts - DIRECT, finish_side)
        later_collect(jnp.int32(later - 1))
        later_sum(jnp.int32(later - 1))
        later_send(jnp.int32(later - 1))
        each(blocks * slices, final)
        sent(jnp.int32(firsts + later - 1), jnp.int32(skip + later - 1), BLOCK)

        each(2 * blocks, lambda q: each(slices, lambda k: to_owner(q, k).wait_send()))

    pl.run_scoped(
        project_phase,
        pltpu.VMEM((width, heads * qkv_head), bf16),
        pltpu.VMEM((2, REPACK, heads, qkv_head), bf16),
    )
    pl.run_scoped(
        attend_phase,
        pltpu.VMEM((2 * BLOCK, qkv_v.shape[0]), f32),
        pltpu.VMEM((2 * BLOCK, wo_v.shape[0]), bf16),
        pltpu.VMEM((2 * BLOCK, h_ref.shape[1]), bf16),
        pltpu.VMEM((BLOCK, width), f32),
        pltpu.VMEM((2, BLOCK, width), f32),
        pltpu.VMEM((BLOCK, width), f32),
        pltpu.VMEM((BLOCK, width // 2), f32),
        pltpu.VMEM((PIECE, width), bf16),
        pltpu.VMEM((PIECE, width), bf16),
    )


def transformer_block(chips, x_loc, ln_gamma, w_qkv, w_out, w_up_t, w_down):
    chunk, width = x_loc.shape
    tokens = chunk * chips * CORES
    heads, qkv_head = w_qkv.shape[1], w_qkv.shape[2]
    ff_width = w_up_t.shape[0]
    arrivals = chunk // PIECE + chunk // PIECE // 2
    firsts = chunk // FIRST
    pieces = chunk // PIECE
    pairs = firsts + (chips - 1) * (chunk // BLOCK)
    per_group = GROUP // PIECE
    bf16, f32 = jnp.bfloat16, jnp.float32
    dma = pltpu.SemaphoreType.DMA
    out = pl.pallas_call(
        functools.partial(block_kernel, chips),
        in_specs=[ANY] * 6,
        out_specs=[ANY] * 7,
        out_shape=[
            jax.ShapeDtypeStruct((chunk, width), bf16),
            jax.ShapeDtypeStruct((tokens, width), bf16),
            jax.ShapeDtypeStruct((tokens, ff_width), bf16),
            jax.ShapeDtypeStruct((chips * chunk, width), f32),
            jax.ShapeDtypeStruct((2 * chunk, width // 2), f32),
            jax.ShapeDtypeStruct((2 * chunk, width), f32),
            jax.ShapeDtypeStruct((chips * chunk, width), f32),
        ],
        scratch_shapes=[
            pltpu.VMEM((tokens, heads * qkv_head), bf16),
            pltpu.VMEM(w_out.shape, bf16),
            pltpu.VMEM(w_down.shape, bf16),
            pltpu.VMEM(w_up_t.shape, bf16),
            pltpu.VMEM((2, GROUP, width), bf16),
            pltpu.VMEM((2, GROUP, ff_width), bf16),
            pltpu.VMEM((1, width), f32),
            dma((4,)), dma((pieces,)), dma((2,)), dma((2, per_group)), dma((2, per_group)),
            dma((arrivals,)), dma((arrivals,)), dma((arrivals,)), dma((arrivals,)),
            dma((2 * arrivals + 1,)), dma((2 * arrivals + 1,)),
            dma((2,)), dma((2,)), dma, dma, dma,
            dma((pairs, 2)), dma((pairs, 2)),
            dma((2, firsts)), dma((2, firsts)),
            dma((2, pieces)), dma((2, pieces)),
        ],
        compiler_params=pltpu.CompilerParams(collective_id=0, has_side_effects=True, vmem_limit_bytes=VMEM_LIMIT),
        name="transformer_block",
    )(x_loc, ln_gamma.reshape(1, width), w_qkv, w_out, w_up_t, w_down)
    return out[0]


def solution(mesh):
    chips = mesh.shape["tp"] // CORES

    def local_block(x_loc, ln_gamma, w_qkv, w_out, w_up, w_down):
        heads, head_dim, model_dim = w_out.shape
        return transformer_block(chips, x_loc, ln_gamma, w_qkv, w_out.reshape(heads * head_dim, model_dim), w_up.T, w_down)

    row_spec = P(("data", "tp"), None)
    return jax.shard_map(local_block, mesh=mesh, in_specs=(row_spec, P(None), P(None, "tp", None), P("tp", None, None), P(None, "tp"), P("tp", None)), out_specs=row_spec, check_vma=False)
```
